32 devices in a mesh: groups: 2 (over y), box: 4 (over z), sub: 2 (over x), rep: 2 (over core).
Axes of the slice: x: 2, y: 2, z: 4, core: 2. Of those that a mesh axis runs over, the one named last changes fastest.
Arguments:
- atom_data: float32 [16, 24, 4, 128], P(('groups', 'box', 'rep')), parts along dimension 0, may hold values from -0.8 to 64, as said below
- atom_type: int32 [16, 24, 128], P(('groups', 'box', 'rep')), parts along dimension 0, may hold values from 0 to 31
- tile_info: int32 [16, 24, 2], P(('groups', 'box', 'rep')), parts along dimension 0, may hold values from 1 to 128, as said below
- lj_repulsion: float32 [32], replicated, may hold values from 100 to 1000
- lj_dispersion: float32 [32], replicated, may hold values from 3 to 30
- send_tiles: int32 [16, 2, 8, 3], P(('groups', 'box', 'rep'), 'sub'), parts along dimension 0, may hold values from 0 to 23, as said below
- send_count: int32 [16, 2, 8], P(('groups', 'box', 'rep'), 'sub'), parts along dimension 0, may hold values from 1 to 3
- pair_slots: int32 [16, 2, 192, 2], P(('groups', 'box', 'rep'), 'sub'), parts along dimension 0, may hold values from 0 to 23, as said below
- pair_count: int32 [16, 2], P(('groups', 'box', 'rep'), 'sub'), parts along dimension 0, may hold values from 1 to 192
Outputs:
- forces: float32 [16, 24, 3, 128], P(('groups', 'box', 'rep'), 'sub'), parts along dimension 0
The draws below stay inside these ranges and needn't reach their ends.
There are 2 independent parts, one for each index of `groups`. The reference program is written for one: setup_inputs(seed, part) draws one part's arguments, and reference() takes and returns one part's arrays. A program takes and returns all parts, laid end to end along the dimension named above; an argument that names none is the same for every part. Nothing has to cross between parts.
Inputs may be any that keep to these rules, and one draw needn't show every extreme that they name: `tile_info`: column 0 lies in 64 to 128, column 1 in 1 to 4. `send_tiles`: the 3 entries of a row are distinct. `pair_slots`: each slot w * 3 + c has c < send_count[w, s, h] for the device (h, s) that holds the pair. `atom_data`: rows 0 to 2 are coordinates in angstrom, row 3 the charge.
All inputs are finite; a program needn't handle non-finite values.
Results may differ from the reference program's by a relative error of at most 0.0003.
Values sent between devices are 32-bit elements; how exact they have to be, the bound alone decides.
No kernel may reach another device: no remote copies, remote signals or barrier semaphores. Data moves between devices by JAX's collectives and lax.ppermute only.
A program may use at most 64 MiB of HBM per device.

```python
import math
import jax
import jax.numpy as jnp
from jax import lax

TILE = 128
HT = 24
CAP = 3
PAIRS_DEV = 192
NTYPE = 32
HOMES = 8
N_SUB = 2
N_REP = 2


def send_counts_of(key):
    counts = jax.random.randint(jax.random.fold_in(key, 101), (HOMES, N_SUB, HOMES), 1, CAP + 1)
    column = jax.random.randint(jax.random.fold_in(key, 102), (N_SUB,), 0, HOMES)
    shifted = jax.random.randint(jax.random.fold_in(key, 103), (), 0, HOMES)
    home_ids = jnp.arange(HOMES)
    full_column = home_ids[None, None, :] == column[None, :, None]
    diagonal = home_ids[None, None, :] == ((home_ids + shifted) % HOMES)[:, None, None]
    return jnp.where(full_column | diagonal, CAP, counts).astype(jnp.int32)


def draw_send_count(key, part):
    return send_counts_of(key)


def draw_send_tiles(key, part):
    scores = jax.random.randint(jax.random.fold_in(key, 104), (HOMES, N_SUB, HOMES, HT), 0, 1 << 20)
    scores = scores * HT + jnp.arange(HT)
    return jnp.argsort(scores, axis=-1)[..., :CAP].astype(jnp.int32)


def draw_pair_slots(key, part):
    counts = send_counts_of(key)
    shape = (HOMES, N_SUB, PAIRS_DEV)
    receiver = jnp.arange(HOMES)[:, None, None]
    plane_ids = jnp.arange(N_SUB)[None, :, None]
    near_home = jax.random.randint(jax.random.fold_in(key, 105), shape, 0, HOMES)
    near_col = jax.random.randint(jax.random.fold_in(key, 106), shape, 0, 1 << 16) % counts[near_home, plane_ids, receiver]
    box_total = HOMES // N_REP
    far_box = jnp.clip(near_home // N_REP + jax.random.randint(jax.random.fold_in(key, 107), shape, -1, 2), 0, box_total - 1)
    far_home = far_box * N_REP + jax.random.randint(jax.random.fold_in(key, 108), shape, 0, N_REP)
    far_col = jax.random.randint(jax.random.fold_in(key, 109), shape, 0, 1 << 16) % counts[far_home, plane_ids, receiver]
    return jnp.stack([near_home * CAP + near_col, far_home * CAP + far_col], axis=-1).astype(jnp.int32)


def draw_pair_count(key, part):
    first_draw = jax.random.randint(jax.random.fold_in(key, 21), (HOMES * N_SUB,), 0, PAIRS_DEV)
    second_draw = jax.random.randint(jax.random.fold_in(key, 22), (HOMES * N_SUB,), 0, PAIRS_DEV)
    counts = 1 + first_draw * second_draw // PAIRS_DEV
    busiest = jax.random.randint(jax.random.fold_in(key, 23), (), 0, HOMES * N_SUB)
    counts = jnp.where(jnp.arange(HOMES * N_SUB) == busiest, PAIRS_DEV, counts)
    return counts.reshape(HOMES, N_SUB).astype(jnp.int32)


def draw_tile_info(key, part):
    present = jax.random.randint(jax.random.fold_in(key, 31), (HOMES, HT), TILE // 2, TILE + 1)
    fullest = jax.random.randint(jax.random.fold_in(key, 32), (HOMES,), 0, HT)
    present = jnp.where(jnp.arange(HT)[None, :] == fullest[:, None], TILE, present)
    run_length = jax.random.randint(jax.random.fold_in(key, 33), (HOMES, HT), 1, 5)
    return jnp.stack([present, run_length], axis=-1).astype(jnp.int32)


def draw_atom_data(key, part):
    unit_cube = jax.random.uniform(jax.random.fold_in(key, 1), (HOMES, HT, 3, TILE), jnp.float32)
    home_ids = jnp.arange(HOMES)
    box_of = (home_ids // N_REP).astype(jnp.float32)[:, None, None]
    rep_of = (home_ids % N_REP).astype(jnp.float32)[:, None, None]
    coord_x = 32.0 * unit_cube[:, :, 0]
    coord_y = 16.0 * (rep_of + unit_cube[:, :, 1])
    coord_z = 16.0 * (box_of + unit_cube[:, :, 2])
    charge = jax.random.uniform(jax.random.fold_in(key, 2), (HOMES, HT, TILE), jnp.float32, -0.8, 0.8)
    return jnp.stack([coord_x, coord_y, coord_z, charge], axis=2).astype(jnp.float32)


def set_ends(values, key, smallest, high):
    place = [jax.random.randint(jax.random.fold_in(key, axis), (), 0, length) for axis, length in enumerate(values.shape)]
    widest = values.shape.index(max(values.shape))
    beside = place[:widest] + [(place[widest] + 1) % values.shape[widest]] + place[widest + 1:]
    return values.at[tuple(place)].set(smallest).at[tuple(beside)].set(high)


def setup_inputs(seed: int = 0, part: int = 0) -> dict:
    keys = jax.random.split(jax.random.key(seed), 10)
    own_keys = jax.random.split(jax.random.fold_in(keys[9], part), 10)
    atom_data = draw_atom_data(jax.random.fold_in(jax.random.fold_in(keys[9], part), 71), part)
    atom_type = set_ends(jax.random.randint(own_keys[1], (HOMES, HT, TILE), 0, NTYPE), jax.random.fold_in(own_keys[1], 1), 0, NTYPE - 1).astype(jnp.int32)
    tile_info = draw_tile_info(jax.random.fold_in(jax.random.fold_in(keys[9], part), 71), part)
    lj_repulsion = jnp.clip(jnp.exp(jax.random.uniform(keys[3], (NTYPE,), jnp.float32, math.log(100.0), math.log(1000.0))), 100.0, 1000.0)
    lj_dispersion = jnp.clip(jnp.exp(jax.random.uniform(keys[4], (NTYPE,), jnp.float32, math.log(3.0), math.log(30.0))), 3.0, 30.0)
    send_tiles = draw_send_tiles(jax.random.fold_in(jax.random.fold_in(keys[9], part), 71), part)
    send_count = draw_send_count(jax.random.fold_in(jax.random.fold_in(keys[9], part), 71), part)
    pair_slots = draw_pair_slots(jax.random.fold_in(jax.random.fold_in(keys[9], part), 71), part)
    pair_count = draw_pair_count(jax.random.fold_in(jax.random.fold_in(keys[9], part), 71), part)
    return {"atom_data": atom_data, "atom_type": atom_type, "tile_info": tile_info, "lj_repulsion": lj_repulsion, "lj_dispersion": lj_dispersion, "send_tiles": send_tiles, "send_count": send_count, "pair_slots": pair_slots, "pair_count": pair_count}


COULOMB = 332.0636
SOFTENING = 9.0
CUTOFF_SQ = 144.0

def pair_forces(near_tile, far_tile, same_tile, near_info, far_info):
    atom_ids = jnp.arange(near_tile.shape[-1], dtype=jnp.int32)
    near_live = atom_ids[None, :] < near_info[:, 0:1]
    far_live = atom_ids[None, :] < far_info[:, 0:1]
    near_mol = atom_ids[None, :] // near_info[:, 1:2]
    far_mol = atom_ids[None, :] // far_info[:, 1:2]
    bonded = same_tile[:, None, None] & (near_mol[:, :, None] == far_mol[:, None, :])
    keeper = near_live[:, :, None] & far_live[:, None, :] & jnp.logical_not(bonded)
    separation = near_tile[:, 0:3, :, None] - far_tile[:, 0:3, None, :]
    dist_sq = lax.optimization_barrier(jnp.sum(separation * separation, axis=1))
    inverse = 1.0 / (dist_sq + SOFTENING)
    inv_cube = inverse * inverse * inverse
    repulsion = near_tile[:, 4, :, None] * far_tile[:, 4, None, :]
    attract = near_tile[:, 5, :, None] * far_tile[:, 5, None, :]
    charges = COULOMB * near_tile[:, 3, :, None] * far_tile[:, 3, None, :]
    rooted = jnp.sqrt(inverse)
    energy = repulsion * inv_cube * inv_cube - attract * inv_cube + charges * rooted
    derivative = (-6.0 * repulsion * inv_cube * inv_cube + 3.0 * attract * inv_cube - 0.5 * charges * rooted) * inverse
    window = jnp.maximum(1.0 - dist_sq / CUTOFF_SQ, 0.0)
    gradient = window * window * derivative - 2.0 / CUTOFF_SQ * window * energy
    weight = jnp.where(keeper, -2.0 * gradient, 0.0)
    return lax.optimization_barrier(jnp.sum(weight[:, None] * separation, axis=-1))

def reference(atom_data, atom_type, tile_info, lj_repulsion, lj_dispersion, send_tiles, send_count, pair_slots, pair_count):
    home_total = atom_data.shape[0]
    tiles_home = atom_data.shape[1]
    tile_width = atom_data.shape[3]
    planes = send_tiles.shape[1]
    capacity = send_tiles.shape[3]
    pairs_each = pair_slots.shape[2]
    repulsion = lj_repulsion[atom_type]
    dispersion = lj_dispersion[atom_type]
    record = jnp.concatenate([atom_data, repulsion[:, :, None], dispersion[:, :, None]], axis=2)
    record = record.reshape(home_total * tiles_home, 6, tile_width)
    tile_meta = tile_info.reshape(home_total * tiles_home, 2)
    receiver = jnp.arange(home_total, dtype=jnp.int32)[:, None, None]
    plane_ids = jnp.arange(planes, dtype=jnp.int32)[None, :, None]

    def locate(slot):
        source = slot // capacity
        column = slot % capacity
        tile_ids = source * tiles_home + send_tiles[source, plane_ids, receiver, column]
        shipped = column < send_count[source, plane_ids, receiver]
        return (tile_ids.astype(jnp.int32), shipped)
    near_slot = pair_slots[..., 0]
    far_slot = pair_slots[..., 1]
    near_ids, near_sent = locate(near_slot)
    far_ids, far_sent = locate(far_slot)
    same_tile = near_slot == far_slot
    active = jnp.arange(pairs_each, dtype=jnp.int32)[None, None, :] < pair_count[:, :, None]

    def flatten(array):
        return array.reshape(home_total * planes, pairs_each)

    def device_pairs(packed):
        near_ids, far_ids, near_sent, far_sent, same_tile, active = packed
        near_meta = jnp.stack([tile_meta[near_ids, 0] * near_sent.astype(jnp.int32), tile_meta[near_ids, 1]], axis=-1)
        far_meta = jnp.stack([tile_meta[far_ids, 0] * far_sent.astype(jnp.int32), tile_meta[far_ids, 1]], axis=-1)
        result = pair_forces(record[near_ids], record[far_ids], same_tile, near_meta, far_meta)
        return jnp.where(active[:, None, None], result, 0.0)
    packed = (flatten(near_ids), flatten(far_ids), flatten(near_sent), flatten(far_sent), flatten(same_tile), flatten(active))
    contributions = lax.map(device_pairs, packed)
    summed = jnp.zeros((home_total * tiles_home, 3, tile_width), jnp.float32)
    summed = summed.at[near_ids.reshape(-1)].add(contributions.reshape(-1, 3, tile_width))
    return summed.reshape(home_total, tiles_home, 3, tile_width)
```

```python
import functools
import math

import jax
import jax.numpy as jnp
from jax import lax
from jax.experimental import pallas as pl
from jax.experimental.pallas import tpu as pltpu
from jax.sharding import PartitionSpec as P

COULOMB = 332.0636
SOFTENING = 9.0
CUTOFF_SQ = 144.0
EDGE = CUTOFF_SQ + SOFTENING
SCALE = EDGE / (CUTOFF_SQ * CUTOFF_SQ)
SCALE_REP = math.sqrt(12.0 * SCALE)
SCALE_DISP = math.sqrt(6.0 * SCALE)
SCALE_CHARGE = math.sqrt(COULOMB * SCALE)
SHIFT_REP = 2.0 / (3.0 * EDGE)
SHIFT_DISP = 1.0 / (3.0 * EDGE)
SHIFT_CHARGE = 3.0 / EDGE
LANES = 128
SUBLANES = 8
CHUNK = 64
UNROLL = 2
SCAN = 8


def ceil_div(a, b):
    return (a + b - 1) // b


def log2_up(n):
    return max(1, (n - 1).bit_length())


class Plan:
    def __init__(self, tiles, pairs, homes, capacity):
        self.tiles, self.pairs, self.homes, self.capacity = tiles, pairs, homes, capacity
        self.pair_rows = ceil_div(pairs, LANES)
        self.home_rows = ceil_div(homes, LANES)
        self.types = 4 * tiles
        self.near = self.types + tiles
        self.far = self.near + self.pair_rows
        self.sends = self.far + self.pair_rows
        self.count = self.sends + capacity * self.home_rows
        self.rows = ceil_div(self.count + 1, SUBLANES) * SUBLANES
        self.tile_bits = log2_up(tiles + 1)
        self.tile_pad = 1 << self.tile_bits
        self.home_pad = ceil_div(homes, SUBLANES) * SUBLANES


def pack_kernel(plan, atom_ref, type_ref, info_ref, send_ref, pair_ref, count_ref, out_ref):
    lane = lax.broadcasted_iota(jnp.int32, (1, LANES), 1)
    lane4 = lax.broadcasted_iota(jnp.int32, (4, LANES), 1)
    row4 = lax.broadcasted_iota(jnp.int32, (4, LANES), 0)
    for t in range(plan.tiles):
        present = info_ref[0, t]
        block = atom_ref[t]
        charge = jnp.where(lane4 < present, block * SCALE_CHARGE, 0.0)
        out_ref[4 * t : 4 * t + 4, :] = jnp.where(row4 == 3, charge, block)
        kinds = jnp.where(lane < present, type_ref[t : t + 1, :], -1)
        out_ref[plan.types + t : plan.types + t + 1, :] = kinds.astype(jnp.float32)
    out_ref[plan.near : plan.rows, :] = jnp.zeros((plan.rows - plan.near, LANES), jnp.float32)
    for r in range(plan.pair_rows):
        width = min(LANES, plan.pairs - r * LANES)
        span = slice(r * LANES, r * LANES + width)
        out_ref[plan.near + r : plan.near + r + 1, 0:width] = pair_ref[0:1, span].astype(jnp.float32)
        out_ref[plan.far + r : plan.far + r + 1, 0:width] = pair_ref[1:2, span].astype(jnp.float32)
    for c in range(plan.capacity):
        for r in range(plan.home_rows):
            width = min(LANES, plan.homes - r * LANES)
            row = plan.sends + c * plan.home_rows + r
            span = slice(r * LANES, r * LANES + width)
            out_ref[row : row + 1, 0:width] = send_ref[c : c + 1, span].astype(jnp.float32)
    counts = jnp.full((1, LANES), count_ref[0, 0], jnp.int32)
    out_ref[plan.count : plan.count + 1, :] = counts.astype(jnp.float32)


def pair_weight(near, far, keep=None):
    dx = near[0] - far[0]
    dy = near[1] - far[1]
    dz = near[2] - far[2]
    soft = dx * dx + dy * dy + (dz * dz + SOFTENING)
    root = lax.rsqrt(soft)
    inverse = root * root
    cube = inverse * inverse * inverse
    edge = jnp.maximum(EDGE - soft, 0.0)
    repulsion = near[4] * far[4] * cube * (inverse - SHIFT_REP)
    attract = near[5] * far[5] * (inverse - SHIFT_DISP)
    charges = near[3] * far[3] * root * (inverse + SHIFT_CHARGE)
    weight = edge * ((repulsion - attract) * cube + charges)
    if keep is not None:
        weight = jnp.where(keep, weight, 0.0)
    return weight * dx, weight * dy, weight * dz


def pair_kernel(
    plan, blocks, sub_total, info_ref, rep_ref, disp_ref, *refs
):
    (payloads, rest) = refs[:blocks], refs[blocks:]
    outs = rest[: 2 if sub_total == 2 else 1]
    (data, rep_rows, disp_rows, code_vm, code_sm, plain, same, far_cols, acc, sem, code_sem) = rest[len(outs) :]
    homes, rows, cap, tiles = plan.homes, plan.rows, plan.capacity, plan.tiles
    replicas = lax.axis_size("rep")
    my_box, my_rep = lax.axis_index("box"), lax.axis_index("rep")
    me = my_box * replicas + my_rep

    copies = []
    if blocks == 1:
        copies.append(pltpu.make_async_copy(payloads[0], data, sem.at[0]))
    else:
        half = blocks // 2
        for n in range(blocks):
            home = (my_box ^ (n % half)) * replicas + (my_rep ^ (n // half))
            target = data.at[pl.ds(pl.multiple_of(home * rows, SUBLANES), rows), :]
            copies.append(pltpu.make_async_copy(payloads[n], target, sem.at[n]))
    for copy in copies:
        copy.start()
    for tile in range(tiles + 1):
        acc[tile] = jnp.zeros((3, SUBLANES, LANES), jnp.float32)
    for copy in copies:
        copy.wait()

    table_rows = []
    for h in range(homes):
        for c in range(cap):
            row = h * rows + plan.sends + c * plan.home_rows
            table_rows.append(data[row : row + 1, :] + float(h * plan.tile_pad))
    slots = len(table_rows)
    padded = ceil_div(slots, LANES) * LANES
    table_rows.append(jnp.zeros((padded - slots, LANES), jnp.float32))
    table = jnp.concatenate(table_rows, axis=0)
    table = jnp.concatenate(
        [table[k * LANES : (k + 1) * LANES, :].T for k in range(padded // LANES)], axis=1
    )[0 : plan.home_pad, :]

    def stacked(offset):
        parts = [data[h * rows + offset : h * rows + offset + 1, :] for h in range(homes)]
        if plan.home_pad > homes:
            parts.append(jnp.zeros((plan.home_pad - homes, LANES), jnp.float32))
        return jnp.concatenate(parts, axis=0)

    counts = stacked(plan.count)
    near_all = [stacked(plan.near + r) for r in range(plan.pair_rows)]
    far_all = [stacked(plan.far + r) for r in range(plan.pair_rows)]
    near_tile = [jnp.zeros_like(counts) for _ in near_all]
    far_tile = [jnp.zeros_like(counts) for _ in near_all]
    for slot in range(slots):
        column = jnp.broadcast_to(table[:, slot : slot + 1], counts.shape)
        for r in range(plan.pair_rows):
            near_tile[r] = jnp.where(near_all[r] == float(slot), column, near_tile[r])
            far_tile[r] = jnp.where(far_all[r] == float(slot), column, far_tile[r])
    lane = lax.broadcasted_iota(jnp.int32, counts.shape, 1)
    counts = counts.astype(jnp.int32)
    mine = me * plan.tile_pad
    for r in range(plan.pair_rows):
        near = near_tile[r].astype(jnp.int32) - mine
        far = far_tile[r].astype(jnp.int32)
        own = (near >= 0) & (near < plan.tile_pad) & (lane + r * LANES < counts)
        equal = near_all[r] == far_all[r]
        flags = jnp.where(own, jnp.where(equal, 2, 1), 0)
        code = far * (plan.tile_pad * 4) + near * 4 + flags
        code_vm[r * plan.home_pad : (r + 1) * plan.home_pad, :] = code
    last = plan.pair_rows * plan.home_pad
    code_vm[last : last + plan.home_pad, :] = counts
    code_copy = pltpu.make_async_copy(code_vm, code_sm, code_sem)
    code_copy.start()

    kinds_total = rep_ref.shape[0]

    def look_up(h, carry):
        first = pl.multiple_of(h * rows + plan.types, SUBLANES)
        kinds = data[pl.ds(first, tiles), :]
        repulsion = jnp.zeros_like(kinds)
        dispersion = jnp.zeros_like(kinds)
        for k in range(kinds_total):
            match = kinds == float(k)
            repulsion = jnp.where(match, rep_ref[k] * SCALE_REP, repulsion)
            dispersion = jnp.where(match, disp_ref[k] * SCALE_DISP, dispersion)
        target = pl.ds(pl.multiple_of(h * plan.tile_pad, SUBLANES), tiles)
        rep_rows[target, :] = repulsion
        disp_rows[target, :] = dispersion
        return carry

    lax.fori_loop(0, homes, look_up, 0)
    code_copy.wait()

    def scan_home(h, ends):
        count = code_sm[last + h, 0]

        def scan_some(step, ends):
            plain_end, same_end = ends
            first = step * SCAN
            row = (first // LANES) * plan.home_pad + h
            column = first % LANES
            for k in range(SCAN):
                code = code_sm[row, column + k]
                plain[plain_end] = code
                same[same_end] = code
                plain_end = plain_end + (code & 1)
                same_end = same_end + ((code >> 1) & 1)
            return plain_end, same_end

        return lax.fori_loop(0, (count + SCAN - 1) // SCAN, scan_some, ends)

    plain_end, same_end = lax.fori_loop(0, homes, scan_home, (jnp.int32(0), jnp.int32(0)))
    for k in range(CHUNK):
        plain[plain_end + k] = tiles * 4

    def decode(code):
        near = (code >> 2) & (plan.tile_pad - 1)
        far = code >> (2 + plan.tile_bits)
        return near, far

    def data_row(tile):
        return (tile >> plan.tile_bits) * rows + (tile & (plan.tile_pad - 1)) * 4

    def turn(code, place):
        _, far = decode(code)
        block = data[pl.ds(data_row(far), 4), :]
        record = jnp.concatenate(
            [
                block,
                rep_rows[pl.ds(far, 1), :],
                disp_rows[pl.ds(far, 1), :],
                jnp.zeros((2, LANES), jnp.float32),
            ],
            axis=0,
        )
        far_cols[place] = record.T

    def compute(code, place, masked):
        near, _ = decode(code)
        own = mine + near
        base = data_row(own)
        wide = (SUBLANES, LANES)
        near_rows = [jnp.broadcast_to(data[pl.ds(base + r, 1), :], wide) for r in range(4)]
        near_rows.append(jnp.broadcast_to(rep_rows[pl.ds(own, 1), :], wide))
        near_rows.append(jnp.broadcast_to(disp_rows[pl.ds(own, 1), :], wide))
        if masked:
            run = info_ref[1, near].astype(jnp.float32)
            share = 1.0 / jnp.full(wide, run, jnp.float32)
            atom_i = lax.broadcasted_iota(jnp.int32, wide, 1).astype(jnp.float32)
            atom_j = lax.broadcasted_iota(jnp.int32, wide, 0).astype(jnp.float32)
            group_i = jnp.floor((atom_i + 0.5) * share)
        total = None
        for step in range(LANES // SUBLANES):
            columns = far_cols[place, step * SUBLANES : (step + 1) * SUBLANES, :]
            far_rows = [jnp.broadcast_to(columns[:, r : r + 1], wide) for r in range(6)]
            keep = None
            if masked:
                group_j = jnp.floor((atom_j + (step * SUBLANES + 0.5)) * share)
                keep = group_i != group_j
            parts = pair_weight(near_rows, far_rows, keep)
            total = parts if total is None else [t + p for t, p in zip(total, parts)]
        return near, total

    def add(near, total):
        for r in range(3):
            acc[near, r] += total[r]

    def do_chunk(chunk, carry):
        first = chunk * CHUNK
        left = jnp.minimum(plain_end - first, CHUNK)

        def turn_some(step, carry):
            for k in range(4):
                turn(plain[first + step * 4 + k], step * 4 + k)
            return carry

        lax.fori_loop(0, (left + 3) // 4, turn_some, 0)

        def pair_some(step, carry):
            done = []
            for k in range(UNROLL):
                place = step * UNROLL + k
                done.append(compute(plain[first + place], place, False))
            for near, total in done:
                add(near, total)
            return carry

        lax.fori_loop(0, (left + UNROLL - 1) // UNROLL, pair_some, 0)
        return carry

    lax.fori_loop(0, (plain_end + CHUNK - 1) // CHUNK, do_chunk, 0)

    def do_same(k, carry):
        turn(same[k], 0)
        near, total = compute(same[k], 0, True)
        add(near, total)
        return carry

    lax.fori_loop(0, same_end, do_same, 0)

    if sub_total == 2:
        half = tiles // 2
        side = lax.axis_index("sub")
        for n in range(2):
            first = (side ^ n) * half
            for t in range(half):
                outs[n][t] = jnp.sum(acc[first + t], axis=1)
    else:
        for t in range(tiles):
            outs[0][t] = jnp.sum(acc[t], axis=1)


def per_device(
    atom_data,
    atom_type,
    tile_info,
    lj_repulsion,
    lj_dispersion,
    send_tiles,
    send_count,
    pair_slots,
    pair_count,
):
    box_total = lax.axis_size("box")
    replicas = lax.axis_size("rep")
    sub_total = lax.axis_size("sub")
    tiles = atom_data.shape[1]
    homes, capacity = send_tiles.shape[2:]
    pairs = pair_slots.shape[2]
    plan = Plan(tiles, pairs, homes, capacity)
    vmem = pl.BlockSpec(memory_space=pltpu.VMEM)
    smem = pl.BlockSpec(memory_space=pltpu.SMEM)
    anywhere = pl.BlockSpec(memory_space=pl.ANY)
    info = tile_info[0].T
    payload = pl.pallas_call(
        functools.partial(pack_kernel, plan),
        out_shape=jax.ShapeDtypeStruct((plan.rows, LANES), jnp.float32),
        in_specs=[vmem, vmem, smem, vmem, vmem, smem],
        out_specs=vmem,
        name="pack",
    )(atom_data[0], atom_type[0], info, send_tiles[0, 0].T, pair_slots[0, 0].T, pair_count)

    fast = replicas == 2 and box_total in (2, 4, 8)
    if fast:
        blocks = [payload]
        for k in range(1, box_total):
            blocks.append(lax.ppermute(payload, "box", [(i, i ^ k) for i in range(box_total)]))
        blocks += [lax.ppermute(block, "rep", [(0, 1), (1, 0)]) for block in blocks]
    else:
        blocks = [lax.all_gather(payload, ("box", "rep"), axis=0, tiled=True)]

    if sub_total == 2:
        outs = [jax.ShapeDtypeStruct((tiles // 2, 3, LANES), jnp.float32)] * 2
    else:
        outs = [jax.ShapeDtypeStruct((tiles, 3, LANES), jnp.float32)]
    code_rows = (plan.pair_rows + 1) * plan.home_pad
    results = pl.pallas_call(
        functools.partial(pair_kernel, plan, len(blocks), sub_total),
        out_shape=outs,
        in_specs=[smem, smem, smem] + [anywhere] * len(blocks),
        out_specs=[vmem] * len(outs),
        scratch_shapes=[
            pltpu.VMEM((homes * plan.rows, LANES), jnp.float32),
            pltpu.VMEM((homes * plan.tile_pad, LANES), jnp.float32),
            pltpu.VMEM((homes * plan.tile_pad, LANES), jnp.float32),
            pltpu.VMEM((code_rows, LANES), jnp.int32),
            pltpu.SMEM((code_rows, LANES), jnp.int32),
            pltpu.SMEM((homes * pairs + CHUNK,), jnp.int32),
            pltpu.SMEM((homes * pairs + CHUNK,), jnp.int32),
            pltpu.VMEM((CHUNK, LANES, SUBLANES), jnp.float32),
            pltpu.VMEM((tiles + 1, 3, SUBLANES, LANES), jnp.float32),
            pltpu.SemaphoreType.DMA((len(blocks),)),
            pltpu.SemaphoreType.DMA,
        ],
        name="pairs",
    )(info, lj_repulsion, lj_dispersion, *blocks)
    if sub_total == 2:
        mine, theirs = results
        arrived = lax.ppermute(theirs, "sub", [(0, 1), (1, 0)])
        return (mine + arrived)[None]
    return lax.psum_scatter(results[0], "sub", scatter_dimension=0, tiled=True)[None]


def solution(mesh):
    placed = (
        P(("groups", "box", "rep"), None, None, None),
        P(("groups", "box", "rep"), None, None),
        P(("groups", "box", "rep"), None, None),
        P(),
        P(),
        P(("groups", "box", "rep"), "sub", None, None),
        P(("groups", "box", "rep"), "sub", None),
        P(("groups", "box", "rep"), "sub", None, None),
        P(("groups", "box", "rep"), "sub"),
    )
    return jax.shard_map(
        per_device,
        mesh=mesh,
        in_specs=placed,
        out_specs=P(("groups", "box", "rep"), "sub", None, None),
        check_vma=False,
    )
```

```python
import functools
import math

import jax
import jax.numpy as jnp
from jax import lax
from jax.experimental import pallas as pl
from jax.experimental.pallas import tpu as pltpu
from jax.sharding import PartitionSpec as P

COULOMB = 332.0636
SOFTENING = 9.0
CUTOFF_SQ = 144.0
EDGE = CUTOFF_SQ + SOFTENING
SCALE = EDGE / (CUTOFF_SQ * CUTOFF_SQ)
SCALE_REP = math.sqrt(12.0 * SCALE)
SCALE_DISP = math.sqrt(6.0 * SCALE)
SCALE_CHARGE = math.sqrt(COULOMB * SCALE)
SHIFT_REP = 2.0 / (3.0 * EDGE)
SHIFT_DISP = 1.0 / (3.0 * EDGE)
SHIFT_CHARGE = 3.0 / EDGE
LANES = 128
SUBLANES = 8
UNROLL = 4
EXCLUDE = 256.0
FAR_GROUP = 1048576.0


def ceil_div(a, b):
    return (a + b - 1) // b


def log2_up(n):
    return max(1, (n - 1).bit_length())


class Plan:
    def __init__(self, tiles, pairs, homes, capacity):
        self.tiles, self.pairs, self.homes, self.capacity = tiles, pairs, homes, capacity
        self.pair_rows = ceil_div(pairs, LANES)
        self.home_rows = ceil_div(homes, LANES)
        self.types = 4 * tiles
        self.near = self.types + tiles
        self.far = self.near + self.pair_rows
        self.sends = self.far + self.pair_rows
        self.count = self.sends + capacity * self.home_rows
        self.rows = ceil_div(self.count + 1, SUBLANES) * SUBLANES
        self.tile_bits = log2_up(tiles + 1)
        self.tile_pad = 1 << self.tile_bits
        self.home_pad = ceil_div(homes, SUBLANES) * SUBLANES


def pack_kernel(plan, atom_ref, type_ref, info_ref, send_ref, pair_ref, count_ref, out_ref):
    lane = lax.broadcasted_iota(jnp.int32, (1, LANES), 1)
    lane4 = lax.broadcasted_iota(jnp.int32, (4, LANES), 1)
    row4 = lax.broadcasted_iota(jnp.int32, (4, LANES), 0)
    for t in range(plan.tiles):
        present = info_ref[0, t]
        block = atom_ref[t]
        charge = jnp.where(lane4 < present, block * SCALE_CHARGE, 0.0)
        out_ref[4 * t : 4 * t + 4, :] = jnp.where(row4 == 3, charge, block)
        kinds = jnp.where(lane < present, type_ref[t : t + 1, :], -1)
        out_ref[plan.types + t : plan.types + t + 1, :] = kinds.astype(jnp.float32)
    out_ref[plan.near : plan.rows, :] = jnp.zeros((plan.rows - plan.near, LANES), jnp.float32)
    for r in range(plan.pair_rows):
        width = min(LANES, plan.pairs - r * LANES)
        span = slice(r * LANES, r * LANES + width)
        out_ref[plan.near + r : plan.near + r + 1, 0:width] = pair_ref[0:1, span].astype(jnp.float32)
        out_ref[plan.far + r : plan.far + r + 1, 0:width] = pair_ref[1:2, span].astype(jnp.float32)
    for c in range(plan.capacity):
        for r in range(plan.home_rows):
            width = min(LANES, plan.homes - r * LANES)
            row = plan.sends + c * plan.home_rows + r
            span = slice(r * LANES, r * LANES + width)
            out_ref[row : row + 1, 0:width] = send_ref[c : c + 1, span].astype(jnp.float32)
    counts = jnp.full((1, LANES), count_ref[0, 0], jnp.int32)
    out_ref[plan.count : plan.count + 1, :] = counts.astype(jnp.float32)


def pair_forces(dx, dy, dz, charge, repulsive, attractive, keep):
    soft = dx * dx + dy * dy + (dz * dz + SOFTENING)
    root = lax.rsqrt(soft)
    inverse = root * root
    cube = inverse * inverse * inverse
    edge = jnp.maximum(jnp.minimum(EDGE - soft, keep), 0.0)
    repulsion = repulsive * cube * (inverse - SHIFT_REP)
    attract = attractive * (inverse - SHIFT_DISP)
    charges = charge * root * (inverse + SHIFT_CHARGE)
    weight = edge * ((repulsion - attract) * cube + charges)
    return weight * dx, weight * dy, weight * dz


def split(values):
    high = values.astype(jnp.bfloat16).astype(jnp.float32)
    rest = values - high
    middle = rest.astype(jnp.bfloat16).astype(jnp.float32)
    low = (rest - middle).astype(jnp.bfloat16).astype(jnp.float32)
    return high, middle, low


def pair_kernel(plan, blocks, sub_total, info_ref, rep_ref, disp_ref, *refs):
    payloads, rest = refs[:blocks], refs[blocks:]
    outs = rest[: 2 if sub_total == 2 else 1]
    (data, rep_rows, disp_rows, groups, near_ops, list_vm, list_sm, acc, sem) = rest[
        len(outs) : len(rest) - 2 * UNROLL
    ]
    sides, products = rest[len(rest) - 2 * UNROLL : len(rest) - UNROLL], rest[len(rest) - UNROLL :]
    homes, rows, cap, tiles = plan.homes, plan.rows, plan.capacity, plan.tiles
    replicas = lax.axis_size("rep")
    my_box, my_rep = lax.axis_index("box"), lax.axis_index("rep")
    me = my_box * replicas + my_rep
    row_ids = lax.broadcasted_iota(jnp.int32, (SUBLANES, LANES), 0)
    lane_ids = lax.broadcasted_iota(jnp.int32, (SUBLANES, LANES), 1)

    if blocks == 1:
        data[...] = payloads[0][...]
    else:
        half = blocks // 2
        for n in range(blocks):
            home = (my_box ^ (n % half)) * replicas + (my_rep ^ (n // half))
            data[pl.ds(pl.multiple_of(home * rows, SUBLANES), rows), :] = payloads[n][...]
    for tile in range(tiles + 1):
        acc[tile] = jnp.zeros((3, SUBLANES, LANES), jnp.float32)

    table_rows = []
    for h in range(homes):
        for c in range(cap):
            row = h * rows + plan.sends + c * plan.home_rows
            table_rows.append(data[row : row + 1, :] + float(h * plan.tile_pad))
    slots = len(table_rows)
    padded = ceil_div(slots, LANES) * LANES
    table_rows.append(jnp.zeros((padded - slots, LANES), jnp.float32))
    table = jnp.concatenate(table_rows, axis=0)
    table = jnp.concatenate(
        [table[k * LANES : (k + 1) * LANES, :].T for k in range(padded // LANES)], axis=1
    )[0 : plan.home_pad, :]

    def stacked(offset):
        parts = [data[h * rows + offset : h * rows + offset + 1, :] for h in range(homes)]
        if plan.home_pad > homes:
            parts.append(jnp.zeros((plan.home_pad - homes, LANES), jnp.float32))
        return jnp.concatenate(parts, axis=0)

    counts = stacked(plan.count)
    near_slot = [stacked(plan.near + r) for r in range(plan.pair_rows)]
    far_slot = [stacked(plan.far + r) for r in range(plan.pair_rows)]
    near_tile = [jnp.zeros_like(counts) for _ in near_slot]
    far_tile = [jnp.zeros_like(counts) for _ in near_slot]
    for slot in range(slots):
        column = jnp.broadcast_to(table[:, slot : slot + 1], counts.shape)
        for r in range(plan.pair_rows):
            near_tile[r] = jnp.where(near_slot[r] == float(slot), column, near_tile[r])
            far_tile[r] = jnp.where(far_slot[r] == float(slot), column, far_tile[r])

    lane_f = lax.broadcasted_iota(jnp.int32, counts.shape, 1).astype(jnp.float32)
    mine = (me * plan.tile_pad).astype(jnp.float32)
    near_all = jnp.concatenate(near_tile, axis=0) - mine
    far_all = jnp.concatenate(far_tile, axis=0)
    same_all = jnp.concatenate(near_slot, axis=0) == jnp.concatenate(far_slot, axis=0)
    ranks = jnp.concatenate([lane_f + float(r * LANES) for r in range(plan.pair_rows)], axis=0)
    limit = jnp.concatenate([counts] * plan.pair_rows, axis=0)
    own = (near_all >= 0.0) & (near_all < float(plan.tile_pad)) & (ranks < limit)
    flags = jnp.where(own, 1.0, 0.0)
    list_rows = flags.shape[0]
    upper = lax.broadcasted_iota(jnp.int32, (LANES, LANES), 0) <= lax.broadcasted_iota(jnp.int32, (LANES, LANES), 1)
    upper = jnp.where(upper, 1.0, 0.0).astype(jnp.bfloat16)
    prefix = jnp.dot(flags.astype(jnp.bfloat16), upper, preferred_element_type=jnp.float32)
    totals = jnp.broadcast_to(jnp.sum(flags, axis=1, keepdims=True), flags.shape)
    below = lax.broadcasted_iota(jnp.int32, (list_rows, list_rows), 0) > lax.broadcasted_iota(
        jnp.int32, (list_rows, list_rows), 1
    )
    below = jnp.where(below, 1.0, 0.0).astype(jnp.bfloat16)
    before = jnp.dot(below, totals.astype(jnp.bfloat16), preferred_element_type=jnp.float32)
    places = jnp.where(own, before + prefix - 1.0, -1.0)
    pair_total = jnp.sum(flags).astype(jnp.int32)
    far_home = jnp.floor((far_all + 0.5) * (1.0 / plan.tile_pad))
    far_in_home = far_all - far_home * float(plan.tile_pad)
    same_f = jnp.where(same_all, 1.0, 0.0)
    wide_rows = lax.broadcasted_iota(jnp.int32, (LANES, LANES), 0).astype(jnp.float32)

    def list_block(block, carry):
        first = (block * LANES).astype(jnp.float32)
        digits = jnp.zeros((SUBLANES, LANES), jnp.float32)
        for r in range(list_rows):
            values = jnp.concatenate(
                [
                    near_all[r : r + 1, :],
                    far_in_home[r : r + 1, :],
                    far_home[r : r + 1, :],
                    same_f[r : r + 1, :],
                    jnp.zeros((SUBLANES - 4, LANES), jnp.float32),
                ],
                axis=0,
            )
            chosen = jnp.broadcast_to(places[r : r + 1, :] - first, (LANES, LANES)) == wide_rows
            chosen = jnp.where(chosen, 1.0, 0.0).astype(jnp.bfloat16)
            digits = digits + lax.dot_general(
                values.astype(jnp.bfloat16),
                chosen,
                (((1,), (1,)), ((), ())),
                preferred_element_type=jnp.float32,
            )
        near, tile, home, same = [digits[k : k + 1, :].astype(jnp.int32) for k in range(4)]
        near = jnp.where(lane_ids[0:1, :] + block * LANES < pair_total, near, tiles)
        code = ((home * plan.tile_pad + tile) * plan.tile_pad + near) * 2 + same
        list_vm[pl.ds(block, 1), :] = code
        return carry

    lax.fori_loop(0, (pair_total + 3 * UNROLL) // LANES + 1, list_block, 0)
    list_copy = pltpu.make_async_copy(list_vm, list_sm, sem)
    list_copy.start()

    kinds_total = rep_ref.shape[0]

    def look_up(h, carry):
        first = pl.multiple_of(h * rows + plan.types, SUBLANES)
        kinds = data[pl.ds(first, tiles), :]
        repulsion = jnp.zeros_like(kinds)
        dispersion = jnp.zeros_like(kinds)
        for k in range(kinds_total):
            match = kinds == float(k)
            repulsion = jnp.where(match, rep_ref[k] * SCALE_REP, repulsion)
            dispersion = jnp.where(match, disp_ref[k] * SCALE_DISP, dispersion)
        target = pl.ds(pl.multiple_of(h * plan.tile_pad, SUBLANES), tiles)
        rep_rows[target, :] = repulsion
        disp_rows[target, :] = dispersion
        return carry

    lax.fori_loop(0, homes, look_up, 0)

    for tile in range(tiles + 1):
        if tile == tiles:
            near_ops[tile] = jnp.zeros(near_ops.shape[1:], jnp.bfloat16)
            groups[tile : tile + 1, :] = jnp.zeros((1, LANES), jnp.float32)
            continue
        run = jnp.full((1, LANES), info_ref[1, tile], jnp.int32).astype(jnp.float32)
        group = jnp.floor((lane_ids[0:1, :].astype(jnp.float32) + 0.5) / run)
        groups[tile : tile + 1, :] = group
        base = pl.multiple_of(me * rows + 4 * tile, 4)
        own_row = me * plan.tile_pad + tile
        record = jnp.concatenate(
            [
                data[pl.ds(base, 4), :],
                rep_rows[pl.ds(own_row, 1), :],
                disp_rows[pl.ds(own_row, 1), :],
                group,
                group * group,
            ],
            axis=0,
        )
        high, middle, low = split(record)
        zero = jnp.zeros_like(record)
        for block in range(7):
            if block < 3:
                minus = jnp.where(row_ids == block, -1.0, 0.0)
                wide = lambda v: jnp.broadcast_to(v[block : block + 1, :], zero.shape)
                ones_side = jnp.where(
                    row_ids == 0, wide(high), jnp.where(row_ids == 1, wide(middle), jnp.where(row_ids == 2, wide(low), 0.0))
                )
                sets = [minus, minus, minus, zero, zero, zero, ones_side, zero]
            elif block < 6:
                pick = lambda v: jnp.where(row_ids == block, v, 0.0)
                sets = [pick(high), pick(high), pick(high), pick(middle), pick(low), pick(middle), zero, zero]
            else:
                wide = lambda v, r: jnp.broadcast_to(v[r : r + 1, :], zero.shape)
                first = jnp.where(row_ids == 6, wide(high, 6) * -2.0, jnp.where(row_ids == 7, 1.0, 0.0))
                second = jnp.where(row_ids == 7, 1.0, 0.0)
                ones_side = jnp.where(row_ids == 0, wide(high, 7), jnp.where(row_ids == 1, wide(middle, 7), 0.0))
                sets = [first * EXCLUDE, second * EXCLUDE, zero, zero, zero, zero, ones_side * EXCLUDE, zero]
            near_ops[tile, :, block * LANES : (block + 1) * LANES] = jnp.concatenate(sets, axis=0).astype(jnp.bfloat16)
    list_copy.wait()

    def decode(place):
        code = list_sm[place // LANES, place % LANES]
        near = (code >> 1) & (plan.tile_pad - 1)
        far = code >> (1 + plan.tile_bits)
        return near, far, code & 1

    ones = jnp.where(row_ids < 3, 1.0, 0.0)

    def far_side(place, target):
        near, far, same = decode(place)
        base = (far >> plan.tile_bits) * rows + (far & (plan.tile_pad - 1)) * 4
        same_row = jnp.full((1, LANES), same, jnp.int32).astype(jnp.float32)
        group = groups[pl.ds(near, 1), :] * same_row
        record = jnp.concatenate(
            [
                data[pl.ds(pl.multiple_of(base, 4), 4), :],
                rep_rows[pl.ds(far, 1), :],
                disp_rows[pl.ds(far, 1), :],
                group,
                group * group + (1.0 - same_row) * FAR_GROUP,
            ],
            axis=0,
        )
        high, middle, low = split(record)
        sides = jnp.concatenate([high, middle, low, high, high, middle, ones, jnp.zeros_like(ones)], axis=0)
        target[...] = sides.astype(jnp.bfloat16).T

    def multiply(place, side, target):
        near, _, _ = decode(place)
        target[...] = jnp.dot(side[...], near_ops[near], preferred_element_type=jnp.float32)

    def add_forces(place, terms):
        near, _, _ = decode(place)
        total = None
        for step in range(LANES // SUBLANES):
            span = slice(step * SUBLANES, (step + 1) * SUBLANES)
            parts = pair_forces(*[terms[span, k * LANES : (k + 1) * LANES] for k in range(7)])
            total = parts if total is None else [t + p for t, p in zip(total, parts)]
        for r in range(3):
            acc[near, r] += total[r]

    for k in range(UNROLL):
        far_side(k, sides[k])
    for k in range(UNROLL):
        multiply(k, sides[k], products[k])
        far_side(UNROLL + k, sides[k])

    def some_pairs(step, carry):
        place = step * UNROLL
        for k in range(UNROLL):
            add_forces(place + k, products[k])
            multiply(place + UNROLL + k, sides[k], products[k])
            far_side(place + 2 * UNROLL + k, sides[k])
        return carry

    lax.fori_loop(0, (pair_total + UNROLL - 1) // UNROLL, some_pairs, 0)

    if sub_total == 2:
        half = tiles // 2
        side = lax.axis_index("sub")
        for n in range(2):
            first = (side ^ n) * half
            for t in range(half):
                outs[n][t] = jnp.sum(acc[first + t], axis=1)
    else:
        for t in range(tiles):
            outs[0][t] = jnp.sum(acc[t], axis=1)


def per_device(
    atom_data,
    atom_type,
    tile_info,
    lj_repulsion,
    lj_dispersion,
    send_tiles,
    send_count,
    pair_slots,
    pair_count,
):
    box_total = lax.axis_size("box")
    replicas = lax.axis_size("rep")
    sub_total = lax.axis_size("sub")
    tiles = atom_data.shape[1]
    homes, capacity = send_tiles.shape[2:]
    pairs = pair_slots.shape[2]
    plan = Plan(tiles, pairs, homes, capacity)
    vmem = pl.BlockSpec(memory_space=pltpu.VMEM)
    smem = pl.BlockSpec(memory_space=pltpu.SMEM)
    info = tile_info[0].T
    payload = pl.pallas_call(
        functools.partial(pack_kernel, plan),
        out_shape=jax.ShapeDtypeStruct((plan.rows, LANES), jnp.float32),
        in_specs=[vmem, vmem, smem, vmem, vmem, smem],
        out_specs=vmem,
        name="pack",
    )(atom_data[0], atom_type[0], info, send_tiles[0, 0].T, pair_slots[0, 0].T, pair_count)

    fast = replicas == 2 and box_total in (2, 4, 8)
    if fast:
        blocks = [payload]
        for k in range(1, box_total):
            blocks.append(lax.ppermute(payload, "box", [(i, i ^ k) for i in range(box_total)]))
        blocks += [lax.ppermute(block, "rep", [(0, 1), (1, 0)]) for block in blocks]
    else:
        blocks = [lax.all_gather(payload, ("box", "rep"), axis=0, tiled=True)]

    if sub_total == 2:
        outs = [jax.ShapeDtypeStruct((tiles // 2, 3, LANES), jnp.float32)] * 2
    else:
        outs = [jax.ShapeDtypeStruct((tiles, 3, LANES), jnp.float32)]
    list_rows = ceil_div(homes * pairs + 3 * UNROLL, LANES) + 1
    results = pl.pallas_call(
        functools.partial(pair_kernel, plan, len(blocks), sub_total),
        out_shape=outs,
        in_specs=[smem, smem, smem] + [vmem] * len(blocks),
        out_specs=[vmem] * len(outs),
        scratch_shapes=[
            pltpu.VMEM((homes * plan.rows, LANES), jnp.float32),
            pltpu.VMEM((homes * plan.tile_pad, LANES), jnp.float32),
            pltpu.VMEM((homes * plan.tile_pad, LANES), jnp.float32),
            pltpu.VMEM((tiles + 1, LANES), jnp.float32),
            pltpu.VMEM((tiles + 1, 8 * SUBLANES, 7 * LANES), jnp.bfloat16),
            pltpu.VMEM((list_rows, LANES), jnp.int32),
            pltpu.SMEM((list_rows, LANES), jnp.int32),
            pltpu.VMEM((tiles + 1, 3, SUBLANES, LANES), jnp.float32),
            pltpu.SemaphoreType.DMA,
        ]
        + [pltpu.VMEM((LANES, 8 * SUBLANES), jnp.bfloat16)] * UNROLL
        + [pltpu.VMEM((LANES, 7 * LANES), jnp.float32)] * UNROLL,
        name="pairs",
    )(info, lj_repulsion, lj_dispersion, *blocks)
    if sub_total == 2:
        mine, theirs = results
        arrived = lax.ppermute(theirs, "sub", [(0, 1), (1, 0)])
        return (mine + arrived)[None]
    return lax.psum_scatter(results[0], "sub", scatter_dimension=0, tiled=True)[None]


def solution(mesh):
    placed = (
        P(("groups", "box", "rep"), None, None, None),
        P(("groups", "box", "rep"), None, None),
        P(("groups", "box", "rep"), None, None),
        P(),
        P(),
        P(("groups", "box", "rep"), "sub", None, None),
        P(("groups", "box", "rep"), "sub", None),
        P(("groups", "box", "rep"), "sub", None, None),
        P(("groups", "box", "rep"), "sub"),
    )
    return jax.shard_map(
        per_device,
        mesh=mesh,
        in_specs=placed,
        out_specs=P(("groups", "box", "rep"), "sub", None, None),
        check_vma=False,
    )
```

```python
import functools
import math

import jax
import jax.numpy as jnp
from jax import lax
from jax.experimental import pallas as pl
from jax.experimental.pallas import tpu as pltpu
from jax.sharding import PartitionSpec as P


COULOMB = 332.0636
SOFTENING = 9.0
CUTOFF_SQ = 144.0
EDGE = CUTOFF_SQ + SOFTENING
SCALE = EDGE / (CUTOFF_SQ * CUTOFF_SQ)
SCALE_REP = math.sqrt(12.0 * SCALE)
SCALE_DISP = math.sqrt(6.0 * SCALE)
SCALE_CHARGE = math.sqrt(COULOMB * SCALE)
SHIFT_REP = 2.0 / (3.0 * EDGE)
SHIFT_DISP = 1.0 / (3.0 * EDGE)
SHIFT_CHARGE = 3.0 / EDGE
LANES = 128
SUBLANES = 8
UNROLL = 4
PREPARE_VMEM = 16 * 1024 * 1024
PAIR_VMEM = 24 * 1024 * 1024
EXCLUDE = 256.0
FAR_GROUP = 1048576.0


def ceil_div(a, b):
    return (a + b - 1) // b


def log2_up(n):
    return max(1, (n - 1).bit_length())


def gathers_by_permute(boxes, replicas):
    return replicas == 2 and boxes in (2, 4, 8)


class Plan:
    def __init__(self, tiles, pairs, homes, capacity):
        self.tiles, self.pairs, self.homes, self.capacity = tiles, pairs, homes, capacity
        self.pair_rows = ceil_div(pairs, LANES)
        self.home_rows = ceil_div(homes, LANES)
        self.types = 4 * tiles
        self.near = self.types + tiles
        self.far = self.near + self.pair_rows
        self.sends = self.far + self.pair_rows
        self.count = self.sends + capacity * self.home_rows
        self.rows = ceil_div(self.count + 1, SUBLANES) * SUBLANES
        self.tile_bits = log2_up(tiles + 1)
        self.tile_pad = 1 << self.tile_bits
        self.home_pad = ceil_div(homes, SUBLANES) * SUBLANES


def pack_kernel(plan, *refs):
    sources, (out_ref, table, groups), targets, sem = refs[:8], refs[8:11], refs[11:19], refs[19]
    copies = [pltpu.make_async_copy(a, b, sem.at[n]) for n, (a, b) in enumerate(zip(sources, targets))]
    for copy in copies:
        copy.start()
    for copy in copies:
        copy.wait()
    atom_ref, type_ref, info_ref, send_ref, pair_ref, count_ref, rep_ref, disp_ref = targets
    lane = lax.broadcasted_iota(jnp.int32, (1, LANES), 1)
    lane4 = lax.broadcasted_iota(jnp.int32, (4, LANES), 1)
    row4 = lax.broadcasted_iota(jnp.int32, (4, LANES), 0)
    for t in range(plan.tiles):
        present = info_ref[0, t]
        block = atom_ref[t]
        charge = jnp.where(lane4 < present, block * SCALE_CHARGE, 0.0)
        out_ref[4 * t : 4 * t + 4, :] = jnp.where(row4 == 3, charge, block)
        kinds = jnp.where(lane < present, type_ref[t : t + 1, :], LANES - 1)
        out_ref[plan.types + t : plan.types + t + 1, :] = kinds.astype(jnp.float32)
    out_ref[plan.near : plan.rows, :] = jnp.zeros((plan.rows - plan.near, LANES), jnp.float32)
    for r in range(plan.pair_rows):
        width = min(LANES, plan.pairs - r * LANES)
        span = slice(r * LANES, r * LANES + width)
        out_ref[plan.near + r : plan.near + r + 1, 0:width] = pair_ref[0:1, span].astype(jnp.float32)
        out_ref[plan.far + r : plan.far + r + 1, 0:width] = pair_ref[1:2, span].astype(jnp.float32)
    for c in range(plan.capacity):
        for r in range(plan.home_rows):
            width = min(LANES, plan.homes - r * LANES)
            row = plan.sends + c * plan.home_rows + r
            span = slice(r * LANES, r * LANES + width)
            out_ref[row : row + 1, 0:width] = send_ref[c, 0:1, span].astype(jnp.float32)
    counts = jnp.full((1, LANES), count_ref[0, 0], jnp.int32)
    out_ref[plan.count : plan.count + 1, :] = counts.astype(jnp.float32)
    lane8 = lax.broadcasted_iota(jnp.int32, (SUBLANES, LANES), 1)
    all_rep = jnp.zeros((SUBLANES, LANES), jnp.float32)
    all_disp = all_rep
    for k in range(rep_ref.shape[0]):
        all_rep = jnp.where(lane8 == k, rep_ref[k] * SCALE_REP, all_rep)
        all_disp = jnp.where(lane8 == k, disp_ref[k] * SCALE_DISP, all_disp)
    table[0:SUBLANES, :] = all_rep
    table[SUBLANES : 2 * SUBLANES, :] = all_disp
    atom = lane.astype(jnp.float32) + 0.5
    for t in range(plan.tiles):
        run = jnp.full((1, LANES), info_ref[1, t], jnp.int32).astype(jnp.float32)
        groups[t : t + 1, :] = jnp.floor(atom / run)
    groups[plan.tiles : plan.tiles + 1, :] = jnp.zeros((1, LANES), jnp.float32)


def pair_forces(dx, dy, dz, charge, repulsive, attractive, keep):
    soft = dx * dx + dy * dy + (dz * dz + SOFTENING)
    root = lax.rsqrt(soft)
    inverse = root * root
    cube = inverse * inverse * inverse
    edge = jnp.maximum(jnp.minimum(EDGE - soft, keep), 0.0)
    repulsion = repulsive * cube * (inverse - SHIFT_REP)
    attract = attractive * (inverse - SHIFT_DISP)
    charges = charge * root * (inverse + SHIFT_CHARGE)
    weight = edge * ((repulsion - attract) * cube + charges)
    return weight * dx, weight * dy, weight * dz


def split(values):
    high = values.astype(jnp.bfloat16).astype(jnp.float32)
    rest = values - high
    middle = rest.astype(jnp.bfloat16).astype(jnp.float32)
    low = (rest - middle).astype(jnp.bfloat16).astype(jnp.float32)
    return high, middle, low


def prepare_kernel(plan, own_ref, table, groups, near_ops):
    tiles = plan.tiles
    row_ids = lax.broadcasted_iota(jnp.int32, (SUBLANES, LANES), 0)
    own_rep, own_disp = [], []
    for first in range(0, tiles, SUBLANES):
        kinds = own_ref[plan.types + first : plan.types + first + SUBLANES, :].astype(jnp.int32)
        own_rep.append(jnp.take_along_axis(table[0:SUBLANES, :], kinds, axis=1))
        own_disp.append(jnp.take_along_axis(table[SUBLANES : 2 * SUBLANES, :], kinds, axis=1))
    own_rep, own_disp = jnp.concatenate(own_rep, axis=0), jnp.concatenate(own_disp, axis=0)

    for tile in range(tiles + 1):
        if tile == tiles:
            near_ops[tile] = jnp.zeros(near_ops.shape[1:], jnp.bfloat16)
            continue
        group = groups[tile : tile + 1, :]
        record = jnp.concatenate(
            [
                own_ref[4 * tile : 4 * tile + 4, :],
                own_rep[tile : tile + 1, :],
                own_disp[tile : tile + 1, :],
                group,
                group * group,
            ],
            axis=0,
        )
        high, middle, low = split(record)
        zero = jnp.zeros_like(record)
        for block in range(7):
            if block < 3:
                minus = jnp.where(row_ids == block, -1.0, 0.0)
                wide = lambda v: jnp.broadcast_to(v[block : block + 1, :], zero.shape)
                ones_side = jnp.where(
                    row_ids == 0, wide(high), jnp.where(row_ids == 1, wide(middle), jnp.where(row_ids == 2, wide(low), 0.0))
                )
                sets = [minus, minus, minus, zero, zero, zero, ones_side, zero]
            elif block < 6:
                pick = lambda v: jnp.where(row_ids == block, v, 0.0)
                sets = [pick(high), pick(high), pick(high), pick(middle), pick(low), pick(middle), zero, zero]
            else:
                wide = lambda v, r: jnp.broadcast_to(v[r : r + 1, :], zero.shape)
                first = jnp.where(row_ids == 6, wide(high, 6) * -2.0, jnp.where(row_ids == 7, 1.0, 0.0))
                second = jnp.where(row_ids == 7, 1.0, 0.0)
                ones_side = jnp.where(row_ids == 0, wide(high, 7), jnp.where(row_ids == 1, wide(middle, 7), 0.0))
                sets = [first * EXCLUDE, second * EXCLUDE, zero, zero, zero, zero, ones_side * EXCLUDE, zero]
            near_ops[tile, :, block * LANES : (block + 1) * LANES] = jnp.concatenate(sets, axis=0).astype(jnp.bfloat16)


def pair_kernel(plan, blocks, sub_total, near_ops, groups, lj_table, *refs):
    payloads, rest = refs[:blocks], refs[blocks:]
    outs = rest[: 2 if sub_total == 2 else 1]
    (data, rep_rows, disp_rows, list_vm, list_sm, acc, sem) = rest[
        len(outs) : len(rest) - 2 * UNROLL
    ]
    sides, products = rest[len(rest) - 2 * UNROLL : len(rest) - UNROLL], rest[len(rest) - UNROLL :]
    homes, rows, cap, tiles = plan.homes, plan.rows, plan.capacity, plan.tiles
    replicas = lax.axis_size("rep")
    my_box, my_rep = lax.axis_index("box"), lax.axis_index("rep")
    me = my_box * replicas + my_rep
    row_ids = lax.broadcasted_iota(jnp.int32, (SUBLANES, LANES), 0)
    lane_ids = lax.broadcasted_iota(jnp.int32, (SUBLANES, LANES), 1)

    def bring(first, last):
        if blocks == 1:
            for h in range(homes):
                data[h * rows + first : h * rows + last, :] = payloads[0][h * rows + first : h * rows + last, :]
            return
        half = blocks // 2
        for n in range(blocks):
            home = (my_box ^ (n % half)) * replicas + (my_rep ^ (n // half))
            start = pl.multiple_of(home * rows, SUBLANES) + first
            data[pl.ds(start, last - first), :] = payloads[n][first:last, :]

    bring(plan.near, rows)

    table_rows = []
    for h in range(homes):
        for c in range(cap):
            row = h * rows + plan.sends + c * plan.home_rows
            table_rows.append(data[row : row + 1, :] + float(h * plan.tile_pad))
    slots = len(table_rows)
    padded = ceil_div(slots, LANES) * LANES
    table_rows.append(jnp.zeros((padded - slots, LANES), jnp.float32))
    table = jnp.concatenate(table_rows, axis=0)
    table = jnp.concatenate(
        [table[k * LANES : (k + 1) * LANES, :].T for k in range(padded // LANES)], axis=1
    )[0 : plan.home_pad, :]

    def stacked(offset):
        parts = [data[h * rows + offset : h * rows + offset + 1, :] for h in range(homes)]
        if plan.home_pad > homes:
            parts.append(jnp.zeros((plan.home_pad - homes, LANES), jnp.float32))
        return jnp.concatenate(parts, axis=0)

    counts = stacked(plan.count)
    near_slot = [stacked(plan.near + r) for r in range(plan.pair_rows)]
    far_slot = [stacked(plan.far + r) for r in range(plan.pair_rows)]
    near_tile = [jnp.zeros_like(counts) for _ in near_slot]
    far_tile = [jnp.zeros_like(counts) for _ in near_slot]
    for slot in range(slots):
        column = jnp.broadcast_to(table[:, slot : slot + 1], counts.shape)
        for r in range(plan.pair_rows):
            near_tile[r] = jnp.where(near_slot[r] == float(slot), column, near_tile[r])
            far_tile[r] = jnp.where(far_slot[r] == float(slot), column, far_tile[r])

    lane_f = lax.broadcasted_iota(jnp.int32, counts.shape, 1).astype(jnp.float32)
    mine = (me * plan.tile_pad).astype(jnp.float32)
    near_all = jnp.concatenate(near_tile, axis=0) - mine
    far_all = jnp.concatenate(far_tile, axis=0)
    same_all = jnp.concatenate(near_slot, axis=0) == jnp.concatenate(far_slot, axis=0)
    ranks = jnp.concatenate([lane_f + float(r * LANES) for r in range(plan.pair_rows)], axis=0)
    limit = jnp.concatenate([counts] * plan.pair_rows, axis=0)
    own = (near_all >= 0.0) & (near_all < float(plan.tile_pad)) & (ranks < limit)
    flags = jnp.where(own, 1.0, 0.0)
    list_rows = flags.shape[0]
    upper = lax.broadcasted_iota(jnp.int32, (LANES, LANES), 0) <= lax.broadcasted_iota(jnp.int32, (LANES, LANES), 1)
    upper = jnp.where(upper, 1.0, 0.0).astype(jnp.bfloat16)
    prefix = jnp.dot(flags.astype(jnp.bfloat16), upper, preferred_element_type=jnp.float32)
    totals = jnp.broadcast_to(jnp.sum(flags, axis=1, keepdims=True), flags.shape)
    below = lax.broadcasted_iota(jnp.int32, (list_rows, list_rows), 0) > lax.broadcasted_iota(
        jnp.int32, (list_rows, list_rows), 1
    )
    below = jnp.where(below, 1.0, 0.0).astype(jnp.bfloat16)
    before = jnp.dot(below, totals.astype(jnp.bfloat16), preferred_element_type=jnp.float32)
    places = jnp.where(own, before + prefix - 1.0, -1.0)
    pair_total = jnp.sum(flags).astype(jnp.int32)
    far_home = jnp.floor((far_all + 0.5) * (1.0 / plan.tile_pad))
    far_in_home = far_all - far_home * float(plan.tile_pad)
    same_f = jnp.where(same_all, 1.0, 0.0)
    wide_rows = lax.broadcasted_iota(jnp.int32, (LANES, LANES), 0).astype(jnp.float32)

    def list_block(block, carry):
        first = (block * LANES).astype(jnp.float32)
        digits = jnp.zeros((SUBLANES, LANES), jnp.float32)
        for r in range(list_rows):
            values = jnp.concatenate(
                [
                    near_all[r : r + 1, :],
                    far_in_home[r : r + 1, :],
                    far_home[r : r + 1, :],
                    same_f[r : r + 1, :],
                    jnp.zeros((SUBLANES - 4, LANES), jnp.float32),
                ],
                axis=0,
            )
            chosen = jnp.broadcast_to(places[r : r + 1, :] - first, (LANES, LANES)) == wide_rows
            chosen = jnp.where(chosen, 1.0, 0.0).astype(jnp.bfloat16)
            digits = digits + lax.dot_general(
                values.astype(jnp.bfloat16),
                chosen,
                (((1,), (1,)), ((), ())),
                preferred_element_type=jnp.float32,
            )
        near, tile, home, same = [digits[k : k + 1, :].astype(jnp.int32) for k in range(4)]
        near = jnp.where(lane_ids[0:1, :] + block * LANES < pair_total, near, tiles)
        code = ((home * plan.tile_pad + tile) * plan.tile_pad + near) * 2 + same
        list_vm[pl.ds(block, 1), :] = code
        return carry

    lax.fori_loop(0, (pair_total + 3 * UNROLL) // LANES + 1, list_block, 0)
    list_copy = pltpu.make_async_copy(list_vm, list_sm, sem)
    list_copy.start()

    bring(0, plan.near)
    for tile in range(tiles + 1):
        acc[tile] = jnp.zeros((3, SUBLANES, LANES), jnp.float32)

    all_rep, all_disp = lj_table[0:SUBLANES, :], lj_table[SUBLANES : 2 * SUBLANES, :]

    def look_up(h, carry):
        for first in range(0, tiles, SUBLANES):
            source = pl.ds(pl.multiple_of(h * rows + plan.types, SUBLANES) + first, SUBLANES)
            kinds = data[source, :].astype(jnp.int32)
            target = pl.ds(pl.multiple_of(h * plan.tile_pad, SUBLANES) + first, SUBLANES)
            rep_rows[target, :] = jnp.take_along_axis(all_rep, kinds, axis=1)
            disp_rows[target, :] = jnp.take_along_axis(all_disp, kinds, axis=1)
        return carry

    if homes <= 8:
        for h in range(homes):
            look_up(h, 0)
    else:
        lax.fori_loop(0, homes, look_up, 0)
    list_copy.wait()

    def decode(place):
        code = list_sm[place // LANES, place % LANES]
        near = (code >> 1) & (plan.tile_pad - 1)
        far = code >> (1 + plan.tile_bits)
        return near, far, code & 1

    ones = jnp.where(row_ids < 3, 1.0, 0.0)

    def far_side(place, target):
        near, far, same = decode(place)
        base = (far >> plan.tile_bits) * rows + (far & (plan.tile_pad - 1)) * 4
        same_row = jnp.full((1, LANES), same, jnp.int32).astype(jnp.float32)
        group = groups[pl.ds(near, 1), :] * same_row
        record = jnp.concatenate(
            [
                data[pl.ds(pl.multiple_of(base, 4), 4), :],
                rep_rows[pl.ds(far, 1), :],
                disp_rows[pl.ds(far, 1), :],
                group,
                group * group + (1.0 - same_row) * FAR_GROUP,
            ],
            axis=0,
        )
        high, middle, low = split(record)
        sides = jnp.concatenate([high, middle, low, high, high, middle, ones, jnp.zeros_like(ones)], axis=0)
        target[...] = sides.astype(jnp.bfloat16).T

    def multiply(place, side, target):
        near, _, _ = decode(place)
        target[...] = jnp.dot(side[...], near_ops[near], preferred_element_type=jnp.float32)

    def add_forces(place, terms):
        near, _, _ = decode(place)
        total = None
        for step in range(LANES // SUBLANES):
            span = slice(step * SUBLANES, (step + 1) * SUBLANES)
            parts = pair_forces(*[terms[span, k * LANES : (k + 1) * LANES] for k in range(7)])
            total = parts if total is None else [t + p for t, p in zip(total, parts)]
        for r in range(3):
            acc[near, r] += total[r]

    for k in range(UNROLL):
        far_side(k, sides[k])
    for k in range(UNROLL):
        multiply(k, sides[k], products[k])
        far_side(UNROLL + k, sides[k])

    def some_pairs(step, carry):
        place = step * UNROLL
        for k in range(UNROLL):
            add_forces(place + k, products[k])
            multiply(place + UNROLL + k, sides[k], products[k])
            far_side(place + 2 * UNROLL + k, sides[k])
        return carry

    lax.fori_loop(0, (pair_total + UNROLL - 1) // UNROLL, some_pairs, 0)

    if sub_total == 2:
        half = tiles // 2
        side = lax.axis_index("sub")
        for n in range(2):
            first = (side ^ n) * half
            for t in range(half):
                for r in range(3):
                    outs[n][3 * t + r] = jnp.sum(acc[first + t, r], axis=0, keepdims=True)
    else:
        for t in range(tiles):
            outs[0][t] = jnp.sum(acc[t], axis=1)


def per_device(
    atom_data,
    atom_type,
    tile_info,
    lj_repulsion,
    lj_dispersion,
    send_tiles,
    send_count,
    pair_slots,
    pair_count,
):
    box_total = lax.axis_size("box")
    replicas = lax.axis_size("rep")
    sub_total = lax.axis_size("sub")
    tiles = atom_data.shape[1]
    homes, capacity = send_tiles.shape[2:]
    pairs = pair_slots.shape[2]
    plan = Plan(tiles, pairs, homes, capacity)
    vmem = pl.BlockSpec(memory_space=pltpu.VMEM)
    smem = pl.BlockSpec(memory_space=pltpu.SMEM)
    hbm = pl.BlockSpec(memory_space=pltpu.HBM)
    info = tile_info[0].T
    raw = (atom_data[0], atom_type[0], info, send_tiles[0].transpose(2, 0, 1), pair_slots[0, 0].T, pair_count)
    raw += (lj_repulsion, lj_dispersion)
    places = (pltpu.VMEM, pltpu.VMEM, pltpu.SMEM, pltpu.VMEM, pltpu.VMEM, pltpu.SMEM, pltpu.SMEM, pltpu.SMEM)
    payload, lj_table, groups = pl.pallas_call(
        functools.partial(pack_kernel, plan),
        out_shape=[
            jax.ShapeDtypeStruct((plan.rows, LANES), jnp.float32),
            jax.ShapeDtypeStruct((2 * SUBLANES, LANES), jnp.float32),
            jax.ShapeDtypeStruct((tiles + 1, LANES), jnp.float32),
        ],
        in_specs=[hbm] * len(raw),
        out_specs=[vmem] * 3,
        scratch_shapes=[place(array.shape, array.dtype) for place, array in zip(places, raw)]
        + [pltpu.SemaphoreType.DMA((len(raw),))],
        name="pack",
    )(*raw)
    near_ops = pl.pallas_call(
        functools.partial(prepare_kernel, plan),
        out_shape=jax.ShapeDtypeStruct((tiles + 1, 8 * SUBLANES, 7 * LANES), jnp.bfloat16),
        in_specs=[vmem] * 3,
        out_specs=vmem,
        compiler_params=pltpu.CompilerParams(vmem_limit_bytes=PREPARE_VMEM),
        cost_estimate=pl.CostEstimate(flops=4000000, bytes_accessed=4000000, transcendentals=0),
        name="prepare",
    )(payload, lj_table, groups)
    tables = (near_ops, groups, lj_table)

    if gathers_by_permute(box_total, replicas):
        blocks = [payload]
        for k in range(1, box_total):
            blocks.append(lax.ppermute(payload, "box", [(i, i ^ k) for i in range(box_total)]))
        for k in range(box_total):
            blocks.append(lax.ppermute(blocks[k], "rep", [(0, 1), (1, 0)]))
    else:
        blocks = [lax.all_gather(payload, ("box", "rep"), axis=0, tiled=True)]

    if sub_total == 2:
        outs = [jax.ShapeDtypeStruct((tiles // 2 * 3, 1, LANES), jnp.float32)] * 2
    else:
        outs = [jax.ShapeDtypeStruct((tiles, 3, LANES), jnp.float32)]
    list_rows = ceil_div(homes * pairs + 3 * UNROLL, LANES) + 1
    results = pl.pallas_call(
        functools.partial(pair_kernel, plan, len(blocks), sub_total),
        out_shape=outs,
        in_specs=[vmem] * (3 + len(blocks)),
        out_specs=[vmem] * len(outs),
        scratch_shapes=[
            pltpu.VMEM((homes * plan.rows, LANES), jnp.float32),
            pltpu.VMEM((homes * plan.tile_pad, LANES), jnp.float32),
            pltpu.VMEM((homes * plan.tile_pad, LANES), jnp.float32),
            pltpu.VMEM((list_rows, LANES), jnp.int32),
            pltpu.SMEM((list_rows, LANES), jnp.int32),
            pltpu.VMEM((tiles + 1, 3, SUBLANES, LANES), jnp.float32),
            pltpu.SemaphoreType.DMA,
        ]
        + [pltpu.VMEM((LANES, 8 * SUBLANES), jnp.bfloat16)] * UNROLL
        + [pltpu.VMEM((LANES, 7 * LANES), jnp.float32)] * UNROLL,
        compiler_params=pltpu.CompilerParams(vmem_limit_bytes=PAIR_VMEM),
        name="pairs",
    )(*tables, *blocks)
    if sub_total == 2:
        mine, theirs = results
        arrived = lax.ppermute(theirs, "sub", [(0, 1), (1, 0)])
        return (mine + arrived).reshape(1, tiles // 2, 3, LANES)
    return lax.psum_scatter(results[0], "sub", scatter_dimension=0, tiled=True)[None]


def solution(mesh):
    placed = (
        P(("groups", "box", "rep"), None, None, None),
        P(("groups", "box", "rep"), None, None),
        P(("groups", "box", "rep"), None, None),
        P(),
        P(),
        P(("groups", "box", "rep"), "sub", None, None),
        P(("groups", "box", "rep"), "sub", None),
        P(("groups", "box", "rep"), "sub", None, None),
        P(("groups", "box", "rep"), "sub"),
    )
    return jax.shard_map(
        per_device,
        mesh=mesh,
        in_specs=placed,
        out_specs=P(("groups", "box", "rep"), "sub", None, None),
        check_vma=False,
    )
```

```python
import functools
import math

import jax
import jax.numpy as jnp
from jax import lax
from jax.experimental import pallas as pl
from jax.experimental.pallas import tpu as pltpu
from jax.sharding import PartitionSpec as P


COULOMB = 332.0636
SOFTENING = 9.0
CUTOFF_SQ = 144.0
EDGE = CUTOFF_SQ + SOFTENING
SCALE = EDGE / (CUTOFF_SQ * CUTOFF_SQ)
SCALE_REP = math.sqrt(12.0 * SCALE)
SCALE_DISP = math.sqrt(6.0 * SCALE)
SCALE_CHARGE = math.sqrt(COULOMB * SCALE)
SHIFT_REP = 2.0 / (3.0 * EDGE)
SHIFT_DISP = 1.0 / (3.0 * EDGE)
SHIFT_CHARGE = 3.0 / EDGE
LANES = 128
SUBLANES = 8
UNROLL = 4
PREPARE_VMEM = 16 * 1024 * 1024
PACK_VMEM = 4 * 1024 * 1024
PAIR_VMEM = 24 * 1024 * 1024
LATE_PAIRS = 28
EXCLUDE = 256.0
FAR_GROUP = 1048576.0


def ceil_div(a, b):
    return (a + b - 1) // b


def log2_up(n):
    return max(1, (n - 1).bit_length())


def gathers_by_permute(boxes, replicas):
    return replicas == 2 and boxes in (2, 4, 8)


class Plan:
    def __init__(self, tiles, pairs, homes, capacity):
        self.tiles, self.pairs, self.homes, self.capacity = tiles, pairs, homes, capacity
        self.pair_rows = ceil_div(pairs, LANES)
        self.home_rows = ceil_div(homes, LANES)
        self.types = 4 * tiles
        self.near = self.types + tiles
        self.far = self.near + self.pair_rows
        self.sends = self.far + self.pair_rows
        self.count = self.sends + capacity * self.home_rows
        self.rows = ceil_div(self.count + 1, SUBLANES) * SUBLANES
        self.tile_bits = log2_up(tiles + 1)
        self.tile_pad = 1 << self.tile_bits
        self.home_pad = ceil_div(homes, SUBLANES) * SUBLANES
        self.list_rows = ceil_div(homes * pairs + 5 * UNROLL, LANES) + 1


def pack_kernel(plan, *refs):
    count_ref, sources, (out_ref, table, groups), targets, sem = refs[0], refs[1:8], refs[8:11], refs[11:18], refs[18]
    copies = [pltpu.make_async_copy(a, b, sem.at[n]) for n, (a, b) in enumerate(zip(sources, targets))]
    for copy in copies:
        copy.start()
    for copy in copies:
        copy.wait()
    atom_ref, type_ref, info_ref, send_ref, pair_ref, rep_ref, disp_ref = targets
    lane = lax.broadcasted_iota(jnp.int32, (1, LANES), 1)
    lane4 = lax.broadcasted_iota(jnp.int32, (4, LANES), 1)
    row4 = lax.broadcasted_iota(jnp.int32, (4, LANES), 0)
    for t in range(plan.tiles):
        present = info_ref[0, t]
        block = atom_ref[t]
        charge = jnp.where(lane4 < present, block * SCALE_CHARGE, 0.0)
        out_ref[4 * t : 4 * t + 4, :] = jnp.where(row4 == 3, charge, block)
        kinds = jnp.where(lane < present, type_ref[t : t + 1, :], LANES - 1)
        out_ref[plan.types + t : plan.types + t + 1, :] = kinds.astype(jnp.float32)
    out_ref[plan.near : plan.rows, :] = jnp.zeros((plan.rows - plan.near, LANES), jnp.float32)
    for r in range(plan.pair_rows):
        width = min(LANES, plan.pairs - r * LANES)
        span = slice(r * LANES, r * LANES + width)
        out_ref[plan.near + r : plan.near + r + 1, 0:width] = pair_ref[0:1, span].astype(jnp.float32)
        out_ref[plan.far + r : plan.far + r + 1, 0:width] = pair_ref[1:2, span].astype(jnp.float32)
    for c in range(plan.capacity):
        for r in range(plan.home_rows):
            width = min(LANES, plan.homes - r * LANES)
            row = plan.sends + c * plan.home_rows + r
            span = slice(r * LANES, r * LANES + width)
            out_ref[row : row + 1, 0:width] = send_ref[c, 0:1, span].astype(jnp.float32)
    counts = jnp.full((1, LANES), count_ref[0, 0], jnp.int32)
    out_ref[plan.count : plan.count + 1, :] = counts.astype(jnp.float32)
    lane8 = lax.broadcasted_iota(jnp.int32, (SUBLANES, LANES), 1)
    all_rep = jnp.zeros((SUBLANES, LANES), jnp.float32)
    all_disp = all_rep
    for k in range(rep_ref.shape[0]):
        all_rep = jnp.where(lane8 == k, rep_ref[k] * SCALE_REP, all_rep)
        all_disp = jnp.where(lane8 == k, disp_ref[k] * SCALE_DISP, all_disp)
    table[0:SUBLANES, :] = all_rep
    table[SUBLANES : 2 * SUBLANES, :] = all_disp
    atom = lane.astype(jnp.float32) + 0.5
    for t in range(plan.tiles):
        run = jnp.full((1, LANES), info_ref[1, t], jnp.int32).astype(jnp.float32)
        groups[t : t + 1, :] = jnp.floor(atom / run)
    groups[plan.tiles : plan.tiles + 1, :] = jnp.zeros((1, LANES), jnp.float32)


def pair_forces(dx, dy, dz, charge, repulsive, attractive, keep):
    soft = dx * dx + dy * dy + (dz * dz + SOFTENING)
    root = lax.rsqrt(soft)
    inverse = root * root
    cube = inverse * inverse * inverse
    edge = jnp.maximum(jnp.minimum(EDGE - soft, keep), 0.0)
    repulsion = repulsive * cube * (inverse - SHIFT_REP)
    attract = attractive * (inverse - SHIFT_DISP)
    charges = charge * root * (inverse + SHIFT_CHARGE)
    weight = edge * ((repulsion - attract) * cube + charges)
    return weight * dx, weight * dy, weight * dz


def split(values):
    high = values.astype(jnp.bfloat16).astype(jnp.float32)
    rest = values - high
    middle = rest.astype(jnp.bfloat16).astype(jnp.float32)
    low = (rest - middle).astype(jnp.bfloat16).astype(jnp.float32)
    return high, middle, low


def prepare_kernel(plan, own_ref, table, groups, near_ops):
    tiles = plan.tiles
    row_ids = lax.broadcasted_iota(jnp.int32, (SUBLANES, LANES), 0)
    own_rep, own_disp = [], []
    for first in range(0, tiles, SUBLANES):
        kinds = own_ref[plan.types + first : plan.types + first + SUBLANES, :].astype(jnp.int32)
        own_rep.append(jnp.take_along_axis(table[0:SUBLANES, :], kinds, axis=1))
        own_disp.append(jnp.take_along_axis(table[SUBLANES : 2 * SUBLANES, :], kinds, axis=1))
    own_rep, own_disp = jnp.concatenate(own_rep, axis=0), jnp.concatenate(own_disp, axis=0)

    for tile in range(tiles + 1):
        if tile == tiles:
            near_ops[tile] = jnp.zeros(near_ops.shape[1:], jnp.bfloat16)
            continue
        group = groups[tile : tile + 1, :]
        record = jnp.concatenate(
            [
                own_ref[4 * tile : 4 * tile + 4, :],
                own_rep[tile : tile + 1, :],
                own_disp[tile : tile + 1, :],
                group,
                group * group,
            ],
            axis=0,
        )
        high, middle, low = split(record)
        zero = jnp.zeros_like(record)
        for block in range(7):
            if block < 3:
                minus = jnp.where(row_ids == block, -1.0, 0.0)
                wide = lambda v: jnp.broadcast_to(v[block : block + 1, :], zero.shape)
                ones_side = jnp.where(
                    row_ids == 0, wide(high), jnp.where(row_ids == 1, wide(middle), jnp.where(row_ids == 2, wide(low), 0.0))
                )
                sets = [minus, minus, minus, zero, zero, zero, ones_side, zero]
            elif block < 6:
                pick = lambda v: jnp.where(row_ids == block, v, 0.0)
                sets = [pick(high), pick(high), pick(high), pick(middle), pick(low), pick(middle), zero, zero]
            else:
                wide = lambda v, r: jnp.broadcast_to(v[r : r + 1, :], zero.shape)
                first = jnp.where(row_ids == 6, wide(high, 6) * -2.0, jnp.where(row_ids == 7, 1.0, 0.0))
                second = jnp.where(row_ids == 7, 1.0, 0.0)
                ones_side = jnp.where(row_ids == 0, wide(high, 7), jnp.where(row_ids == 1, wide(middle, 7), 0.0))
                sets = [first * EXCLUDE, second * EXCLUDE, zero, zero, zero, zero, ones_side * EXCLUDE, zero]
            near_ops[tile, :, block * LANES : (block + 1) * LANES] = jnp.concatenate(sets, axis=0).astype(jnp.bfloat16)


def pair_kernel(plan, blocks, halves, near_ops, groups, lj_table, *refs):
    payloads, rest = refs[:blocks], refs[blocks:]
    (out, early, list_sm, data, rep_rows, disp_rows), rest = rest[:6], rest[6:]
    sides, products, (list_vm, acc, sem) = rest[:UNROLL], rest[UNROLL : 2 * UNROLL], rest[2 * UNROLL :]
    homes, rows, cap, tiles = plan.homes, plan.rows, plan.capacity, plan.tiles
    replicas = lax.axis_size("rep")
    my_box, my_rep = lax.axis_index("box"), lax.axis_index("rep")
    me = my_box * replicas + my_rep
    row_ids = lax.broadcasted_iota(jnp.int32, (SUBLANES, LANES), 0)
    lane_ids = lax.broadcasted_iota(jnp.int32, (SUBLANES, LANES), 1)

    def bring(first, last):
        if blocks == 1:
            for h in range(homes):
                data[h * rows + first : h * rows + last, :] = payloads[0][h * rows + first : h * rows + last, :]
            return
        half = blocks // 2
        for n in range(blocks):
            home = (my_box ^ (n % half)) * replicas + (my_rep ^ (n // half))
            start = pl.multiple_of(home * rows, SUBLANES) + first
            data[pl.ds(start, last - first), :] = payloads[n][first:last, :]

    bring(plan.near, rows)

    table_rows = []
    for h in range(homes):
        for c in range(cap):
            row = h * rows + plan.sends + c * plan.home_rows
            table_rows.append(data[row : row + 1, :] + float(h * plan.tile_pad))
    slots = len(table_rows)
    padded = ceil_div(slots, LANES) * LANES
    table_rows.append(jnp.zeros((padded - slots, LANES), jnp.float32))
    table = jnp.concatenate(table_rows, axis=0)
    table = jnp.concatenate(
        [table[k * LANES : (k + 1) * LANES, :].T for k in range(padded // LANES)], axis=1
    )[0 : plan.home_pad, :]

    def stacked(offset):
        parts = [data[h * rows + offset : h * rows + offset + 1, :] for h in range(homes)]
        if plan.home_pad > homes:
            parts.append(jnp.zeros((plan.home_pad - homes, LANES), jnp.float32))
        return jnp.concatenate(parts, axis=0)

    counts = stacked(plan.count)
    near_slot = [stacked(plan.near + r) for r in range(plan.pair_rows)]
    far_slot = [stacked(plan.far + r) for r in range(plan.pair_rows)]
    near_tile = [jnp.zeros_like(counts) for _ in near_slot]
    far_tile = [jnp.zeros_like(counts) for _ in near_slot]
    for slot in range(slots):
        column = jnp.broadcast_to(table[:, slot : slot + 1], counts.shape)
        for r in range(plan.pair_rows):
            near_tile[r] = jnp.where(near_slot[r] == float(slot), column, near_tile[r])
            far_tile[r] = jnp.where(far_slot[r] == float(slot), column, far_tile[r])

    lane_f = lax.broadcasted_iota(jnp.int32, counts.shape, 1).astype(jnp.float32)
    mine = (me * plan.tile_pad).astype(jnp.float32)
    near_all = jnp.concatenate(near_tile, axis=0) - mine
    far_all = jnp.concatenate(far_tile, axis=0)
    same_all = jnp.concatenate(near_slot, axis=0) == jnp.concatenate(far_slot, axis=0)
    ranks = jnp.concatenate([lane_f + float(r * LANES) for r in range(plan.pair_rows)], axis=0)
    limit = jnp.concatenate([counts] * plan.pair_rows, axis=0)
    own = (near_all >= 0.0) & (near_all < float(plan.tile_pad)) & (ranks < limit)
    list_rows = own.shape[0]
    if halves:
        half = tiles // 2
        side = lax.axis_index("sub")
        kept = jnp.where(side == 0, near_all, float(tiles - 1) - near_all) < float(half)
        segments = [own & jnp.logical_not(kept), own & kept]
    else:
        segments = [own]
    flags = jnp.concatenate([jnp.where(segment, 1.0, 0.0) for segment in segments], axis=0)
    flag_rows = flags.shape[0]
    upper = lax.broadcasted_iota(jnp.int32, (LANES, LANES), 0) <= lax.broadcasted_iota(jnp.int32, (LANES, LANES), 1)
    upper = jnp.where(upper, 1.0, 0.0).astype(jnp.bfloat16)
    prefix = jnp.dot(flags.astype(jnp.bfloat16), upper, preferred_element_type=jnp.float32)
    totals = jnp.broadcast_to(jnp.sum(flags, axis=1, keepdims=True), flags.shape)
    below = lax.broadcasted_iota(jnp.int32, (flag_rows, flag_rows), 0) > lax.broadcasted_iota(
        jnp.int32, (flag_rows, flag_rows), 1
    )
    below = jnp.where(below, 1.0, 0.0).astype(jnp.bfloat16)
    before = jnp.dot(below, totals.astype(jnp.bfloat16), preferred_element_type=jnp.float32)
    ranked = before + prefix - 1.0
    pair_total = jnp.sum(flags).astype(jnp.int32)
    places = jnp.where(segments[0], ranked[0:list_rows, :], -1.0)
    first_total = pair_total
    if halves:
        places = jnp.where(segments[1], ranked[list_rows:, :], places)
        theirs = jnp.sum(flags[0:list_rows, :]).astype(jnp.int32)
        first_total = jnp.maximum(theirs, pair_total - LATE_PAIRS)
    first_total = (first_total + (UNROLL - 1)) // UNROLL * UNROLL
    far_home = jnp.floor((far_all + 0.5) * (1.0 / plan.tile_pad))
    far_in_home = far_all - far_home * float(plan.tile_pad)
    same_f = jnp.where(same_all, 1.0, 0.0)
    wide_rows = lax.broadcasted_iota(jnp.int32, (LANES, LANES), 0).astype(jnp.float32)

    def list_block(block, carry):
        first = (block * LANES).astype(jnp.float32)
        digits = jnp.zeros((SUBLANES, LANES), jnp.float32)
        for r in range(list_rows):
            values = jnp.concatenate(
                [
                    near_all[r : r + 1, :],
                    far_in_home[r : r + 1, :],
                    far_home[r : r + 1, :],
                    same_f[r : r + 1, :],
                    jnp.ones((1, LANES), jnp.float32),
                    jnp.zeros((SUBLANES - 5, LANES), jnp.float32),
                ],
                axis=0,
            )
            chosen = jnp.broadcast_to(places[r : r + 1, :] - first, (LANES, LANES)) == wide_rows
            chosen = jnp.where(chosen, 1.0, 0.0).astype(jnp.bfloat16)
            digits = digits + lax.dot_general(
                values.astype(jnp.bfloat16),
                chosen,
                (((1,), (1,)), ((), ())),
                preferred_element_type=jnp.float32,
            )
        near, tile, home, same, used = [digits[k : k + 1, :].astype(jnp.int32) for k in range(5)]
        near = jnp.where(used > 0, near, tiles)
        code = ((home * plan.tile_pad + tile) * plan.tile_pad + near) * 2 + same
        list_vm[pl.ds(block, 1), :] = code
        return carry

    lax.fori_loop(0, (pair_total + 4 * UNROLL) // LANES + 1, list_block, 0)
    list_copy = pltpu.make_async_copy(list_vm, list_sm.at[0 : plan.list_rows], sem)
    list_copy.start()

    bring(0, plan.near)

    all_rep, all_disp = lj_table[0:SUBLANES, :], lj_table[SUBLANES : 2 * SUBLANES, :]

    def look_up(h, carry):
        for first in range(0, tiles, SUBLANES):
            source = pl.ds(pl.multiple_of(h * rows + plan.types, SUBLANES) + first, SUBLANES)
            kinds = data[source, :].astype(jnp.int32)
            target = pl.ds(pl.multiple_of(h * plan.tile_pad, SUBLANES) + first, SUBLANES)
            rep_rows[target, :] = jnp.take_along_axis(all_rep, kinds, axis=1)
            disp_rows[target, :] = jnp.take_along_axis(all_disp, kinds, axis=1)
        return carry

    if homes <= 8:
        for h in range(homes):
            look_up(h, 0)
    else:
        lax.fori_loop(0, homes, look_up, 0)
    list_copy.wait()
    list_sm[plan.list_rows, 0] = first_total
    list_sm[plan.list_rows, 1] = jnp.maximum(pair_total - first_total, 0)
    run_pairs(plan, near_ops, groups, data, rep_rows, disp_rows, list_sm, acc, sides, products, 0, first_total)
    if halves:
        side = lax.axis_index("sub")
        write_forces(acc, out, (side ^ 1) * (tiles // 2), tiles // 2)
        write_forces(acc, early, side * (tiles // 2), tiles // 2)
    else:
        write_forces(acc, out, 0, tiles)


def second_kernel(plan, near_ops, groups, early, list_sm, data, rep_rows, disp_rows, *refs):
    out, acc = refs[2 * UNROLL], refs[-1]
    sides, products = refs[2 * UNROLL + 1 : 3 * UNROLL + 1], refs[3 * UNROLL + 1 : -1]
    start, total = list_sm[plan.list_rows, 0], list_sm[plan.list_rows, 1]
    run_pairs(plan, near_ops, groups, data, rep_rows, disp_rows, list_sm, acc, sides, products, start, total, False)
    write_forces(acc, out, lax.axis_index("sub") * (plan.tiles // 2), plan.tiles // 2, early)


def write_forces(acc, out, first, count, early=None):
    for t in range(count):
        for r in range(3):
            total = jnp.sum(acc[first + t, r], axis=0, keepdims=True)
            out[3 * t + r] = total if early is None else total + early[3 * t + r]


def run_pairs(plan, near_ops, groups, data, rep_rows, disp_rows, list_sm, acc, sides, products, start, total, fill=True):
    rows, tiles = plan.rows, plan.tiles
    row_ids = lax.broadcasted_iota(jnp.int32, (SUBLANES, LANES), 0)
    for tile in range(tiles + 1):
        acc[tile] = jnp.zeros((3, SUBLANES, LANES), jnp.float32)

    def decode(place):
        code = list_sm[place // LANES, place % LANES]
        near = (code >> 1) & (plan.tile_pad - 1)
        far = code >> (1 + plan.tile_bits)
        return near, far, code & 1

    ones = jnp.where(row_ids < 3, 1.0, 0.0)

    def far_side(place, target):
        near, far, same = decode(place)
        base = (far >> plan.tile_bits) * rows + (far & (plan.tile_pad - 1)) * 4
        same_row = jnp.full((1, LANES), same, jnp.int32).astype(jnp.float32)
        group = groups[pl.ds(near, 1), :] * same_row
        record = jnp.concatenate(
            [
                data[pl.ds(pl.multiple_of(base, 4), 4), :],
                rep_rows[pl.ds(far, 1), :],
                disp_rows[pl.ds(far, 1), :],
                group,
                group * group + (1.0 - same_row) * FAR_GROUP,
            ],
            axis=0,
        )
        high, middle, low = split(record)
        sides = jnp.concatenate([high, middle, low, high, high, middle, ones, jnp.zeros_like(ones)], axis=0)
        target[...] = sides.astype(jnp.bfloat16).T

    def multiply(place, side, target):
        near, _, _ = decode(place)
        target[...] = jnp.dot(side[...], near_ops[near], preferred_element_type=jnp.float32)

    def add_forces(place, terms):
        near, _, _ = decode(place)
        total = None
        for step in range(LANES // SUBLANES):
            span = slice(step * SUBLANES, (step + 1) * SUBLANES)
            parts = pair_forces(*[terms[span, k * LANES : (k + 1) * LANES] for k in range(7)])
            total = parts if total is None else [t + p for t, p in zip(total, parts)]
        for r in range(3):
            acc[near, r] += total[r]

    if fill:
        for k in range(UNROLL):
            far_side(start + k, sides[k])
        for k in range(UNROLL):
            multiply(start + k, sides[k], products[k])
            far_side(start + UNROLL + k, sides[k])

    def some_pairs(step, carry):
        place = start + step * UNROLL
        for k in range(UNROLL):
            add_forces(place + k, products[k])
            multiply(place + UNROLL + k, sides[k], products[k])
            far_side(place + 2 * UNROLL + k, sides[k])
        return carry

    lax.fori_loop(0, (total + UNROLL - 1) // UNROLL, some_pairs, 0)


def per_device(
    atom_data,
    atom_type,
    tile_info,
    lj_repulsion,
    lj_dispersion,
    send_tiles,
    send_count,
    pair_slots,
    pair_count,
):
    box_total = lax.axis_size("box")
    replicas = lax.axis_size("rep")
    sub_total = lax.axis_size("sub")
    tiles = atom_data.shape[1]
    homes, capacity = send_tiles.shape[2:]
    pairs = pair_slots.shape[2]
    plan = Plan(tiles, pairs, homes, capacity)
    vmem = pl.BlockSpec(memory_space=pltpu.VMEM)
    smem = pl.BlockSpec(memory_space=pltpu.SMEM)
    hbm = pl.BlockSpec(memory_space=pltpu.HBM)
    info = tile_info[0].T
    raw = (atom_data[0], atom_type[0], info, send_tiles[0].transpose(2, 0, 1), pair_slots[0, 0].T)
    raw += (lj_repulsion, lj_dispersion)
    places = (pltpu.VMEM, pltpu.VMEM, pltpu.SMEM, pltpu.VMEM, pltpu.VMEM, pltpu.SMEM, pltpu.SMEM)
    payload, lj_table, groups = pl.pallas_call(
        functools.partial(pack_kernel, plan),
        out_shape=[
            pltpu.VMEM((plan.rows, LANES), jnp.float32),
            pltpu.VMEM((2 * SUBLANES, LANES), jnp.float32),
            pltpu.VMEM((tiles + 1, LANES), jnp.float32),
        ],
        in_specs=[smem] + [hbm] * len(raw),
        out_specs=[vmem] * 3,
        scratch_shapes=[place(array.shape, array.dtype) for place, array in zip(places, raw)]
        + [pltpu.SemaphoreType.DMA((len(raw),))],
        compiler_params=pltpu.CompilerParams(vmem_limit_bytes=PACK_VMEM),
        name="pack",
    )(pair_count, *[pltpu.with_memory_space_constraint(array, pltpu.HBM) for array in raw])
    near_ops = pl.pallas_call(
        functools.partial(prepare_kernel, plan),
        out_shape=jax.ShapeDtypeStruct((tiles + 1, 8 * SUBLANES, 7 * LANES), jnp.bfloat16),
        in_specs=[vmem] * 3,
        out_specs=vmem,
        compiler_params=pltpu.CompilerParams(vmem_limit_bytes=PREPARE_VMEM),
        cost_estimate=pl.CostEstimate(flops=4000000, bytes_accessed=4000000, transcendentals=0),
        name="prepare",
    )(payload, lj_table, groups)
    tables = (near_ops, groups, lj_table)

    if gathers_by_permute(box_total, replicas):
        blocks = [payload]
        for k in range(1, box_total):
            blocks.append(lax.ppermute(payload, "box", [(i, i ^ k) for i in range(box_total)]))
        for k in range(box_total):
            blocks.append(lax.ppermute(blocks[k], "rep", [(0, 1), (1, 0)]))
    else:
        blocks = [lax.all_gather(payload, ("box", "rep"), axis=0, tiled=True)]

    halves = sub_total == 2
    count = tiles // 2 if halves else tiles
    forces = jax.ShapeDtypeStruct((count * 3, 1, LANES), jnp.float32)
    sums = pltpu.VMEM((tiles + 1, 3, SUBLANES, LANES), jnp.float32)
    buffers = [jax.ShapeDtypeStruct((LANES, 8 * SUBLANES), jnp.bfloat16)] * UNROLL
    buffers += [jax.ShapeDtypeStruct((LANES, 7 * LANES), jnp.float32)] * UNROLL
    results, *state = pl.pallas_call(
        functools.partial(pair_kernel, plan, len(blocks), halves),
        out_shape=[
            forces,
            forces,
            jax.ShapeDtypeStruct((plan.list_rows + 1, LANES), jnp.int32),
            jax.ShapeDtypeStruct((homes * plan.rows, LANES), jnp.float32),
            jax.ShapeDtypeStruct((homes * plan.tile_pad, LANES), jnp.float32),
            jax.ShapeDtypeStruct((homes * plan.tile_pad, LANES), jnp.float32),
        ]
        + buffers,
        in_specs=[vmem] * (3 + len(blocks)),
        out_specs=[vmem] * 2 + [smem] + [vmem] * (3 + len(buffers)),
        scratch_shapes=[pltpu.VMEM((plan.list_rows, LANES), jnp.int32), sums, pltpu.SemaphoreType.DMA],
        compiler_params=pltpu.CompilerParams(vmem_limit_bytes=PAIR_VMEM),
        name="pairs",
    )(*tables, *blocks)
    if not halves:
        results = results.reshape(tiles, 3, LANES)
        return lax.psum_scatter(results, "sub", scatter_dimension=0, tiled=True)[None]
    arrived = lax.ppermute(results, "sub", [(0, 1), (1, 0)])
    first = 7
    mine, *_ = pl.pallas_call(
        functools.partial(second_kernel, plan),
        out_shape=[forces] + buffers,
        in_specs=[vmem] * 3 + [smem] + [vmem] * (3 + len(buffers)),
        out_specs=[vmem] * (1 + len(buffers)),
        input_output_aliases={first + k: 1 + k for k in range(len(buffers))},
        scratch_shapes=[sums],
        compiler_params=pltpu.CompilerParams(vmem_limit_bytes=PAIR_VMEM),
        cost_estimate=pl.CostEstimate(flops=20000000, bytes_accessed=4000000, transcendentals=0),
        name="second",
    )(near_ops, groups, *state)
    return (mine + arrived).reshape(1, count, 3, LANES)


def solution(mesh):
    placed = (
        P(("groups", "box", "rep"), None, None, None),
        P(("groups", "box", "rep"), None, None),
        P(("groups", "box", "rep"), None, None),
        P(),
        P(),
        P(("groups", "box", "rep"), "sub", None, None),
        P(("groups", "box", "rep"), "sub", None),
        P(("groups", "box", "rep"), "sub", None, None),
        P(("groups", "box", "rep"), "sub"),
    )
    return jax.shard_map(
        per_device,
        mesh=mesh,
        in_specs=placed,
        out_specs=P(("groups", "box", "rep"), "sub", None, None),
        check_vma=False,
    )
```

```python
import functools
import math

import jax
import jax.numpy as jnp
from jax import lax
from jax.experimental import pallas as pl
from jax.experimental.pallas import tpu as pltpu
from jax.sharding import PartitionSpec as P


COULOMB = 332.0636
SOFTENING = 9.0
CUTOFF_SQ = 144.0
EDGE = CUTOFF_SQ + SOFTENING
SCALE = EDGE / (CUTOFF_SQ * CUTOFF_SQ)
SCALE_REP = math.sqrt(12.0 * SCALE)
SCALE_DISP = math.sqrt(6.0 * SCALE)
SCALE_CHARGE = math.sqrt(COULOMB * SCALE)
SHIFT_REP = 2.0 / (3.0 * EDGE)
SHIFT_DISP = 1.0 / (3.0 * EDGE)
SHIFT_CHARGE = 3.0 / EDGE
LANES = 128
SUBLANES = 8
UNROLL = 6
PREPARE_VMEM = 16 * 1024 * 1024
PACK_VMEM = 4 * 1024 * 1024
PAIR_VMEM = 24 * 1024 * 1024
LATE_PAIRS = 36
COUNT_LANE = 64
FEW_ROWS = 96
EXCLUDE = 256.0
FAR_GROUP = 1048576.0


def ceil_div(a, b):
    return (a + b - 1) // b


def log2_up(n):
    return max(1, (n - 1).bit_length())


def gathers_by_permute(boxes, replicas):
    return replicas == 2 and boxes in (2, 4, 8)


class Plan:
    def __init__(self, tiles, pairs, homes, capacity):
        self.tiles, self.pairs, self.homes, self.capacity = tiles, pairs, homes, capacity
        self.pair_rows = ceil_div(pairs, LANES)
        self.home_rows = ceil_div(homes, LANES)
        self.classes = homes <= LANES - COUNT_LANE
        self.types = 4 * tiles
        self.near = self.types + tiles
        self.far = self.near + self.pair_rows
        self.sends = self.far + self.pair_rows
        self.count = self.sends + capacity * self.home_rows
        self.rows = ceil_div(self.count + 1, SUBLANES) * SUBLANES
        self.tile_bits = log2_up(tiles + 1)
        self.tile_pad = 1 << self.tile_bits
        self.home_pad = ceil_div(homes, SUBLANES) * SUBLANES
        self.list_rows = ceil_div(homes * pairs + 5 * UNROLL, LANES) + 1


def pack_kernel(plan, *refs):
    count_ref, sources, (out_ref, table, groups), targets, sem = refs[0], refs[1:8], refs[8:11], refs[11:18], refs[18]
    copies = [pltpu.make_async_copy(a, b, sem.at[n]) for n, (a, b) in enumerate(zip(sources, targets))]
    for copy in copies:
        copy.start()
    for copy in copies:
        copy.wait()
    atom_ref, type_ref, info_ref, send_ref, pair_ref, rep_ref, disp_ref = targets
    lane = lax.broadcasted_iota(jnp.int32, (1, LANES), 1)
    lane4 = lax.broadcasted_iota(jnp.int32, (4, LANES), 1)
    row4 = lax.broadcasted_iota(jnp.int32, (4, LANES), 0)
    for t in range(plan.tiles):
        present = info_ref[0, t]
        block = atom_ref[t]
        charge = jnp.where(lane4 < present, block * SCALE_CHARGE, 0.0)
        out_ref[4 * t : 4 * t + 4, :] = jnp.where(row4 == 3, charge, block)
        kinds = jnp.where(lane < present, type_ref[t : t + 1, :], LANES - 1)
        out_ref[plan.types + t : plan.types + t + 1, :] = kinds.astype(jnp.float32)
    out_ref[plan.near : plan.rows, :] = jnp.zeros((plan.rows - plan.near, LANES), jnp.float32)
    for r in range(plan.pair_rows):
        width = min(LANES, plan.pairs - r * LANES)
        span = slice(r * LANES, r * LANES + width)
        out_ref[plan.near + r : plan.near + r + 1, 0:width] = pair_ref[0:1, span].astype(jnp.float32)
        out_ref[plan.far + r : plan.far + r + 1, 0:width] = pair_ref[1:2, span].astype(jnp.float32)
    for c in range(plan.capacity):
        for r in range(plan.home_rows):
            width = min(LANES, plan.homes - r * LANES)
            row = plan.sends + c * plan.home_rows + r
            span = slice(r * LANES, r * LANES + width)
            chosen = send_ref[c, 0:1, span]
            out_ref[row : row + 1, 0:width] = chosen.astype(jnp.float32)
            if plan.classes:
                present = jnp.zeros_like(chosen)
                for t in range(plan.tiles):
                    present = jnp.where(chosen == t, info_ref[0, t], present)
                out_ref[row : row + 1, COUNT_LANE : COUNT_LANE + width] = present.astype(jnp.float32)
    counts = jnp.full((1, LANES), count_ref[0, 0], jnp.int32)
    out_ref[plan.count : plan.count + 1, :] = counts.astype(jnp.float32)
    lane8 = lax.broadcasted_iota(jnp.int32, (SUBLANES, LANES), 1)
    all_rep = jnp.zeros((SUBLANES, LANES), jnp.float32)
    all_disp = all_rep
    for k in range(rep_ref.shape[0]):
        all_rep = jnp.where(lane8 == k, rep_ref[k] * SCALE_REP, all_rep)
        all_disp = jnp.where(lane8 == k, disp_ref[k] * SCALE_DISP, all_disp)
    table[0:SUBLANES, :] = all_rep
    table[SUBLANES : 2 * SUBLANES, :] = all_disp
    atom = lane.astype(jnp.float32) + 0.5
    for t in range(plan.tiles):
        run = jnp.full((1, LANES), info_ref[1, t], jnp.int32).astype(jnp.float32)
        groups[t : t + 1, :] = jnp.floor(atom / run)
    groups[plan.tiles : plan.tiles + 1, :] = jnp.zeros((1, LANES), jnp.float32)


def pair_forces(dx, dy, dz, charge, repulsive, attractive, keep):
    soft = dx * dx + dy * dy + (dz * dz + SOFTENING)
    root = lax.rsqrt(soft)
    inverse = root * root
    cube = inverse * inverse * inverse
    edge = jnp.maximum(jnp.minimum(EDGE - soft, keep), 0.0)
    repulsion = repulsive * cube * (inverse - SHIFT_REP)
    attract = attractive * (inverse - SHIFT_DISP)
    charges = charge * root * (inverse + SHIFT_CHARGE)
    weight = edge * ((repulsion - attract) * cube + charges)
    return weight * dx, weight * dy, weight * dz


def split(values):
    high = values.astype(jnp.bfloat16).astype(jnp.float32)
    rest = values - high
    middle = rest.astype(jnp.bfloat16).astype(jnp.float32)
    low = (rest - middle).astype(jnp.bfloat16).astype(jnp.float32)
    return high, middle, low


def prepare_kernel(plan, own_ref, table, groups, near_ops):
    tiles = plan.tiles
    row_ids = lax.broadcasted_iota(jnp.int32, (SUBLANES, LANES), 0)
    own_rep, own_disp = [], []
    for first in range(0, tiles, SUBLANES):
        kinds = own_ref[plan.types + first : plan.types + first + SUBLANES, :].astype(jnp.int32)
        own_rep.append(jnp.take_along_axis(table[0:SUBLANES, :], kinds, axis=1))
        own_disp.append(jnp.take_along_axis(table[SUBLANES : 2 * SUBLANES, :], kinds, axis=1))
    own_rep, own_disp = jnp.concatenate(own_rep, axis=0), jnp.concatenate(own_disp, axis=0)

    for tile in range(tiles + 1):
        if tile == tiles:
            near_ops[tile] = jnp.zeros(near_ops.shape[1:], jnp.bfloat16)
            continue
        group = groups[tile : tile + 1, :]
        record = jnp.concatenate(
            [
                own_ref[4 * tile : 4 * tile + 4, :],
                own_rep[tile : tile + 1, :],
                own_disp[tile : tile + 1, :],
                group,
                group * group,
            ],
            axis=0,
        )
        high, middle, low = split(record)
        zero = jnp.zeros_like(record)
        for block in range(7):
            if block < 3:
                minus = jnp.where(row_ids == block, -1.0, 0.0)
                wide = lambda v: jnp.broadcast_to(v[block : block + 1, :], zero.shape)
                ones_side = jnp.where(
                    row_ids == 0, wide(high), jnp.where(row_ids == 1, wide(middle), jnp.where(row_ids == 2, wide(low), 0.0))
                )
                sets = [minus, minus, minus, zero, zero, zero, ones_side, zero]
            elif block < 6:
                pick = lambda v: jnp.where(row_ids == block, v, 0.0)
                sets = [pick(high), pick(high), pick(high), pick(middle), pick(low), pick(middle), zero, zero]
            else:
                wide = lambda v, r: jnp.broadcast_to(v[r : r + 1, :], zero.shape)
                first = jnp.where(row_ids == 6, wide(high, 6) * -2.0, jnp.where(row_ids == 7, 1.0, 0.0))
                second = jnp.where(row_ids == 7, 1.0, 0.0)
                ones_side = jnp.where(row_ids == 0, wide(high, 7), jnp.where(row_ids == 1, wide(middle, 7), 0.0))
                sets = [first * EXCLUDE, second * EXCLUDE, zero, zero, zero, zero, ones_side * EXCLUDE, zero]
            near_ops[tile, :, block * LANES : (block + 1) * LANES] = jnp.concatenate(sets, axis=0).astype(jnp.bfloat16)


def pair_kernel(plan, blocks, halves, near_ops, groups, lj_table, *refs):
    payloads, rest = refs[:blocks], refs[blocks:]
    (out, early, list_sm, data, rep_rows, disp_rows), rest = rest[:6], rest[6:]
    sides, products, (list_vm, acc, sem) = rest[:UNROLL], rest[UNROLL : 2 * UNROLL], rest[2 * UNROLL :]
    homes, rows, cap, tiles = plan.homes, plan.rows, plan.capacity, plan.tiles
    replicas = lax.axis_size("rep")
    my_box, my_rep = lax.axis_index("box"), lax.axis_index("rep")
    me = my_box * replicas + my_rep
    row_ids = lax.broadcasted_iota(jnp.int32, (SUBLANES, LANES), 0)
    lane_ids = lax.broadcasted_iota(jnp.int32, (SUBLANES, LANES), 1)

    def bring(first, last):
        if blocks == 1:
            for h in range(homes):
                data[h * rows + first : h * rows + last, :] = payloads[0][h * rows + first : h * rows + last, :]
            return
        half = blocks // 2
        for n in range(blocks):
            home = (my_box ^ (n % half)) * replicas + (my_rep ^ (n // half))
            start = pl.multiple_of(home * rows, SUBLANES) + first
            data[pl.ds(start, last - first), :] = payloads[n][first:last, :]

    bring(plan.near, rows)

    table_rows = []
    for h in range(homes):
        for c in range(cap):
            row = h * rows + plan.sends + c * plan.home_rows
            table_rows.append(data[row : row + 1, :] + float(h * plan.tile_pad))
    slots = len(table_rows)
    padded = ceil_div(slots, LANES) * LANES
    table_rows.append(jnp.zeros((padded - slots, LANES), jnp.float32))
    table = jnp.concatenate(table_rows, axis=0)
    table = jnp.concatenate(
        [table[k * LANES : (k + 1) * LANES, :].T for k in range(padded // LANES)], axis=1
    )
    present = table[COUNT_LANE : COUNT_LANE + plan.home_pad, :]
    table = table[0 : plan.home_pad, :]

    def stacked(offset):
        parts = [data[h * rows + offset : h * rows + offset + 1, :] for h in range(homes)]
        if plan.home_pad > homes:
            parts.append(jnp.zeros((plan.home_pad - homes, LANES), jnp.float32))
        return jnp.concatenate(parts, axis=0)

    counts = stacked(plan.count)
    near_slot = [stacked(plan.near + r) for r in range(plan.pair_rows)]
    far_slot = [stacked(plan.far + r) for r in range(plan.pair_rows)]
    near_tile = [jnp.zeros_like(counts) for _ in near_slot]
    far_tile = [jnp.zeros_like(counts) for _ in near_slot]
    far_few = [jnp.zeros_like(counts) for _ in near_slot]
    for slot in range(slots):
        column = jnp.broadcast_to(table[:, slot : slot + 1], counts.shape)
        for r in range(plan.pair_rows):
            near_tile[r] = jnp.where(near_slot[r] == float(slot), column, near_tile[r])
            far_tile[r] = jnp.where(far_slot[r] == float(slot), column, far_tile[r])
        if plan.classes:
            atoms = jnp.broadcast_to(present[:, slot : slot + 1], counts.shape) - float(slot // cap * plan.tile_pad)
            for r in range(plan.pair_rows):
                far_few[r] = jnp.where(far_slot[r] == float(slot), atoms, far_few[r])

    lane_f = lax.broadcasted_iota(jnp.int32, counts.shape, 1).astype(jnp.float32)
    mine = (me * plan.tile_pad).astype(jnp.float32)
    near_all = jnp.concatenate(near_tile, axis=0) - mine
    far_all = jnp.concatenate(far_tile, axis=0)
    same_all = jnp.concatenate(near_slot, axis=0) == jnp.concatenate(far_slot, axis=0)
    ranks = jnp.concatenate([lane_f + float(r * LANES) for r in range(plan.pair_rows)], axis=0)
    limit = jnp.concatenate([counts] * plan.pair_rows, axis=0)
    own = (near_all >= 0.0) & (near_all < float(plan.tile_pad)) & (ranks < limit)
    list_rows = own.shape[0]
    if halves:
        half = tiles // 2
        side = lax.axis_index("sub")
        kept = jnp.where(side == 0, near_all, float(tiles - 1) - near_all) < float(half)
        theirs, ours = own & jnp.logical_not(kept), own & kept
    else:
        theirs, ours = own, None
    few = jnp.concatenate(far_few, axis=0)
    few = (few > 0.0) & (few <= float(FEW_ROWS))
    many = jnp.logical_not(few)
    segments = [theirs & many, theirs & few]
    if halves:
        segments += [ours & few, ours & many]
    flags = jnp.concatenate([jnp.where(segment, 1.0, 0.0) for segment in segments], axis=0)
    flag_rows = flags.shape[0]
    upper = lax.broadcasted_iota(jnp.int32, (LANES, LANES), 0) <= lax.broadcasted_iota(jnp.int32, (LANES, LANES), 1)
    upper = jnp.where(upper, 1.0, 0.0).astype(jnp.bfloat16)
    prefix = jnp.dot(flags.astype(jnp.bfloat16), upper, preferred_element_type=jnp.float32)
    totals = jnp.broadcast_to(jnp.sum(flags, axis=1, keepdims=True), flags.shape)
    below = lax.broadcasted_iota(jnp.int32, (flag_rows, flag_rows), 0) > lax.broadcasted_iota(
        jnp.int32, (flag_rows, flag_rows), 1
    )
    below = jnp.where(below, 1.0, 0.0).astype(jnp.bfloat16)
    before = jnp.dot(below, totals.astype(jnp.bfloat16), preferred_element_type=jnp.float32)
    ranked = before + prefix - 1.0
    places = jnp.full(own.shape, -1.0, jnp.float32)
    sizes = []
    for n, segment in enumerate(segments):
        span = slice(n * list_rows, (n + 1) * list_rows)
        places = jnp.where(segment, ranked[span, :], places)
        sizes.append(jnp.sum(flags[span, :]).astype(jnp.int32))
    pair_total = sum(sizes)
    first_total = pair_total
    if halves:
        first_total = jnp.maximum(sizes[0] + sizes[1], pair_total - LATE_PAIRS)
    first_total = (first_total + (UNROLL - 1)) // UNROLL * UNROLL
    few_start = (sizes[0] + (UNROLL - 1)) // UNROLL * UNROLL
    few_end = (pair_total - (sizes[3] if halves else 0)) // UNROLL * UNROLL
    some_few = few_end - few_start >= UNROLL
    few_start = jnp.where(some_few, few_start, 0)
    few_end = jnp.where(some_few, few_end, 0)
    few_last = jnp.where(some_few, few_end - UNROLL, 0)
    far_home = jnp.floor((far_all + 0.5) * (1.0 / plan.tile_pad))
    far_in_home = far_all - far_home * float(plan.tile_pad)
    same_f = jnp.where(same_all, 1.0, 0.0)
    wide_rows = lax.broadcasted_iota(jnp.int32, (LANES, LANES), 0).astype(jnp.float32)

    def list_block(block, carry):
        first = (block * LANES).astype(jnp.float32)
        digits = jnp.zeros((SUBLANES, LANES), jnp.float32)
        for r in range(list_rows):
            values = jnp.concatenate(
                [
                    near_all[r : r + 1, :],
                    far_in_home[r : r + 1, :],
                    far_home[r : r + 1, :],
                    same_f[r : r + 1, :],
                    jnp.ones((1, LANES), jnp.float32),
                    jnp.zeros((SUBLANES - 5, LANES), jnp.float32),
                ],
                axis=0,
            )
            chosen = jnp.broadcast_to(places[r : r + 1, :] - first, (LANES, LANES)) == wide_rows
            chosen = jnp.where(chosen, 1.0, 0.0).astype(jnp.bfloat16)
            digits = digits + lax.dot_general(
                values.astype(jnp.bfloat16),
                chosen,
                (((1,), (1,)), ((), ())),
                preferred_element_type=jnp.float32,
            )
        near, tile, home, same, used = [digits[k : k + 1, :].astype(jnp.int32) for k in range(5)]
        near = jnp.where(used > 0, near, tiles)
        code = ((home * plan.tile_pad + tile) * plan.tile_pad + near) * 2 + same
        list_vm[pl.ds(block, 1), :] = code
        return carry

    lax.fori_loop(0, (pair_total + 4 * UNROLL) // LANES + 1, list_block, 0)
    list_copy = pltpu.make_async_copy(list_vm, list_sm.at[0 : plan.list_rows], sem)
    list_copy.start()

    bring(0, plan.near)

    all_rep, all_disp = lj_table[0:SUBLANES, :], lj_table[SUBLANES : 2 * SUBLANES, :]

    def look_up(h, carry):
        for first in range(0, tiles, SUBLANES):
            source = pl.ds(pl.multiple_of(h * rows + plan.types, SUBLANES) + first, SUBLANES)
            kinds = data[source, :].astype(jnp.int32)
            target = pl.ds(pl.multiple_of(h * plan.tile_pad, SUBLANES) + first, SUBLANES)
            rep_rows[target, :] = jnp.take_along_axis(all_rep, kinds, axis=1)
            disp_rows[target, :] = jnp.take_along_axis(all_disp, kinds, axis=1)
        return carry

    if homes <= 8:
        for h in range(homes):
            look_up(h, 0)
    else:
        lax.fori_loop(0, homes, look_up, 0)
    list_copy.wait()
    for k, bound in enumerate((first_total, pair_total, few_start, few_last, few_end)):
        list_sm[plan.list_rows, k] = bound
    buffers = (list_sm, acc, sides, products)
    stops = [jnp.minimum(bound, first_total) for bound in (few_start, few_last, few_end, first_total)]
    steps = [(0, stops[0], LANES, LANES), (stops[0], stops[1], FEW_ROWS, FEW_ROWS)]
    steps += [(stops[1], stops[2], FEW_ROWS, LANES), (stops[2], stops[3], LANES, LANES)]
    run_pairs(plan, near_ops, groups, data, rep_rows, disp_rows, *buffers, steps, True)
    if halves:
        side = lax.axis_index("sub")
        write_forces(acc, out, (side ^ 1) * (tiles // 2), tiles // 2)
        write_forces(acc, early, side * (tiles // 2), tiles // 2)
    else:
        write_forces(acc, out, 0, tiles)


def second_kernel(plan, near_ops, groups, early, list_sm, data, rep_rows, disp_rows, *refs):
    out, acc = refs[2 * UNROLL], refs[-1]
    sides, products = refs[2 * UNROLL + 1 : 3 * UNROLL + 1], refs[3 * UNROLL + 1 : -1]
    start, total, *bounds = [list_sm[plan.list_rows, k] for k in range(5)]
    stops = [jnp.maximum(bound, start) for bound in bounds]
    end = jnp.maximum((total + (UNROLL - 1)) // UNROLL * UNROLL, stops[2])
    steps = [(stops[0], stops[1], FEW_ROWS, FEW_ROWS), (stops[1], stops[2], FEW_ROWS, LANES)]
    steps.append((stops[2], end, LANES, LANES))
    run_pairs(plan, near_ops, groups, data, rep_rows, disp_rows, list_sm, acc, sides, products, steps, False)
    write_forces(acc, out, lax.axis_index("sub") * (plan.tiles // 2), plan.tiles // 2, early)


def write_forces(acc, out, first, count, early=None):
    for t in range(count):
        for r in range(3):
            total = jnp.sum(acc[first + t, r], axis=0, keepdims=True)
            out[3 * t + r] = total if early is None else total + early[3 * t + r]


def run_pairs(plan, near_ops, groups, data, rep_rows, disp_rows, list_sm, acc, sides, products, steps, fill):
    rows, tiles = plan.rows, plan.tiles
    row_ids = lax.broadcasted_iota(jnp.int32, (SUBLANES, LANES), 0)
    for tile in range(tiles + 1):
        acc[tile] = jnp.zeros((3, SUBLANES, LANES), jnp.float32)

    def decode(place):
        code = list_sm[place // LANES, place % LANES]
        near = (code >> 1) & (plan.tile_pad - 1)
        far = code >> (1 + plan.tile_bits)
        return near, far, code & 1

    ones = jnp.where(row_ids < 3, 1.0, 0.0)

    def far_side(place, target):
        near, far, same = decode(place)
        base = (far >> plan.tile_bits) * rows + (far & (plan.tile_pad - 1)) * 4
        same_row = jnp.full((1, LANES), same, jnp.int32).astype(jnp.float32)
        group = groups[pl.ds(near, 1), :] * same_row
        record = jnp.concatenate(
            [
                data[pl.ds(pl.multiple_of(base, 4), 4), :],
                rep_rows[pl.ds(far, 1), :],
                disp_rows[pl.ds(far, 1), :],
                group,
                group * group + (1.0 - same_row) * FAR_GROUP,
            ],
            axis=0,
        )
        high, middle, low = split(record)
        sides = jnp.concatenate([high, middle, low, high, high, middle, ones, jnp.zeros_like(ones)], axis=0)
        target[...] = sides.astype(jnp.bfloat16).T

    def multiply(place, side, target, live):
        near, _, _ = decode(place)
        target[0:live, :] = jnp.dot(side[0:live, :], near_ops[near], preferred_element_type=jnp.float32)

    def add_forces(place, terms, live):
        near, _, _ = decode(place)
        total = None
        for step in range(live // SUBLANES):
            span = slice(step * SUBLANES, (step + 1) * SUBLANES)
            parts = pair_forces(*[terms[span, k * LANES : (k + 1) * LANES] for k in range(7)])
            total = parts if total is None else [t + p for t, p in zip(total, parts)]
        for r in range(3):
            acc[near, r] += total[r]

    if fill:
        for k in range(UNROLL):
            far_side(k, sides[k])
        for k in range(UNROLL):
            multiply(k, sides[k], products[k], LANES)
            far_side(UNROLL + k, sides[k])

    for first, stop, live, live_next in steps:

        def some_pairs(step, carry, first=first, live=live, live_next=live_next):
            place = first + step * UNROLL
            for k in range(UNROLL):
                add_forces(place + k, products[k], live)
                multiply(place + UNROLL + k, sides[k], products[k], live_next)
                far_side(place + 2 * UNROLL + k, sides[k])
            return carry

        lax.fori_loop(0, (stop - first) // UNROLL, some_pairs, 0)


def per_device(
    atom_data,
    atom_type,
    tile_info,
    lj_repulsion,
    lj_dispersion,
    send_tiles,
    send_count,
    pair_slots,
    pair_count,
):
    box_total = lax.axis_size("box")
    replicas = lax.axis_size("rep")
    sub_total = lax.axis_size("sub")
    tiles = atom_data.shape[1]
    homes, capacity = send_tiles.shape[2:]
    pairs = pair_slots.shape[2]
    plan = Plan(tiles, pairs, homes, capacity)
    vmem = pl.BlockSpec(memory_space=pltpu.VMEM)
    smem = pl.BlockSpec(memory_space=pltpu.SMEM)
    hbm = pl.BlockSpec(memory_space=pltpu.HBM)
    info = tile_info[0].T
    raw = (atom_data[0], atom_type[0], info, send_tiles[0].transpose(2, 0, 1), pair_slots[0, 0].T)
    raw += (lj_repulsion, lj_dispersion)
    places = (pltpu.VMEM, pltpu.VMEM, pltpu.SMEM, pltpu.VMEM, pltpu.VMEM, pltpu.SMEM, pltpu.SMEM)
    payload, lj_table, groups = pl.pallas_call(
        functools.partial(pack_kernel, plan),
        out_shape=[
            pltpu.VMEM((plan.rows, LANES), jnp.float32),
            pltpu.VMEM((2 * SUBLANES, LANES), jnp.float32),
            pltpu.VMEM((tiles + 1, LANES), jnp.float32),
        ],
        in_specs=[smem] + [hbm] * len(raw),
        out_specs=[vmem] * 3,
        scratch_shapes=[place(array.shape, array.dtype) for place, array in zip(places, raw)]
        + [pltpu.SemaphoreType.DMA((len(raw),))],
        compiler_params=pltpu.CompilerParams(vmem_limit_bytes=PACK_VMEM),
        name="pack",
    )(pair_count, *[pltpu.with_memory_space_constraint(array, pltpu.HBM) for array in raw])
    near_ops = pl.pallas_call(
        functools.partial(prepare_kernel, plan),
        out_shape=jax.ShapeDtypeStruct((tiles + 1, 8 * SUBLANES, 7 * LANES), jnp.bfloat16),
        in_specs=[vmem] * 3,
        out_specs=vmem,
        compiler_params=pltpu.CompilerParams(vmem_limit_bytes=PREPARE_VMEM),
        cost_estimate=pl.CostEstimate(flops=4000000, bytes_accessed=4000000, transcendentals=0),
        name="prepare",
    )(payload, lj_table, groups)
    tables = (near_ops, groups, lj_table)

    if gathers_by_permute(box_total, replicas):
        blocks = [payload]
        for k in range(1, box_total):
            blocks.append(lax.ppermute(payload, "box", [(i, i ^ k) for i in range(box_total)]))
        for k in range(box_total):
            blocks.append(lax.ppermute(blocks[k], "rep", [(0, 1), (1, 0)]))
    else:
        blocks = [lax.all_gather(payload, ("box", "rep"), axis=0, tiled=True)]

    halves = sub_total == 2
    count = tiles // 2 if halves else tiles
    forces = jax.ShapeDtypeStruct((count * 3, 1, LANES), jnp.float32)
    sums = pltpu.VMEM((tiles + 1, 3, SUBLANES, LANES), jnp.float32)
    buffers = [jax.ShapeDtypeStruct((LANES, 8 * SUBLANES), jnp.bfloat16)] * UNROLL
    buffers += [jax.ShapeDtypeStruct((LANES, 7 * LANES), jnp.float32)] * UNROLL
    results, *state = pl.pallas_call(
        functools.partial(pair_kernel, plan, len(blocks), halves),
        out_shape=[
            forces,
            forces,
            jax.ShapeDtypeStruct((plan.list_rows + 1, LANES), jnp.int32),
            jax.ShapeDtypeStruct((homes * plan.rows, LANES), jnp.float32),
            jax.ShapeDtypeStruct((homes * plan.tile_pad, LANES), jnp.float32),
            jax.ShapeDtypeStruct((homes * plan.tile_pad, LANES), jnp.float32),
        ]
        + buffers,
        in_specs=[vmem] * (3 + len(blocks)),
        out_specs=[vmem] * 2 + [smem] + [vmem] * (3 + len(buffers)),
        scratch_shapes=[pltpu.VMEM((plan.list_rows, LANES), jnp.int32), sums, pltpu.SemaphoreType.DMA],
        compiler_params=pltpu.CompilerParams(vmem_limit_bytes=PAIR_VMEM),
        name="pairs",
    )(*tables, *blocks)
    if not halves:
        results = results.reshape(tiles, 3, LANES)
        return lax.psum_scatter(results, "sub", scatter_dimension=0, tiled=True)[None]
    arrived = lax.ppermute(results, "sub", [(0, 1), (1, 0)])
    first = 7
    mine, *_ = pl.pallas_call(
        functools.partial(second_kernel, plan),
        out_shape=[forces] + buffers,
        in_specs=[vmem] * 3 + [smem] + [vmem] * (3 + len(buffers)),
        out_specs=[vmem] * (1 + len(buffers)),
        input_output_aliases={first + k: 1 + k for k in range(len(buffers))},
        scratch_shapes=[sums],
        compiler_params=pltpu.CompilerParams(vmem_limit_bytes=PAIR_VMEM),
        cost_estimate=pl.CostEstimate(flops=20000000, bytes_accessed=4000000, transcendentals=0),
        name="second",
    )(near_ops, groups, *state)
    return (mine + arrived).reshape(1, count, 3, LANES)


def solution(mesh):
    placed = (
        P(("groups", "box", "rep"), None, None, None),
        P(("groups", "box", "rep"), None, None),
        P(("groups", "box", "rep"), None, None),
        P(),
        P(),
        P(("groups", "box", "rep"), "sub", None, None),
        P(("groups", "box", "rep"), "sub", None),
        P(("groups", "box", "rep"), "sub", None, None),
        P(("groups", "box", "rep"), "sub"),
    )
    return jax.shard_map(
        per_device,
        mesh=mesh,
        in_specs=placed,
        out_specs=P(("groups", "box", "rep"), "sub", None, None),
        check_vma=False,
    )
```
